32 devices in a mesh: dp: 8 (over z, core), expert: 4 (over y, x).
Axes of the slice: x: 2, y: 2, z: 4, core: 2. Of those that a mesh axis runs over, the one named last changes fastest.
Arguments:
- attention_gradient: bfloat16 [8, 6144, 1024], P('dp', None, 'expert')
- attention_weight: float32 [6144, 1024], P('dp', 'expert'), may hold values from -6 to 6
- attention_mean: float32 [6144, 1024], P('dp', 'expert'), may hold values from -0.0012 to 0.0012
- attention_square: float32 [6144, 1024], P('dp', 'expert'), may hold values from 1e-09 to 1e-07
- expert_gradient: float32 [8, 4, 8, 6144], P('dp', 'expert')
- expert_weight: float32 [8, 4, 8, 6144], P('dp', 'expert'), may hold values from -6 to 6
- held_mean: float32 [8, 32, 6144], P('dp', 'expert'), may hold values from -0.0006 to 0.0006
- held_square: float32 [8, 32, 6144], P('dp', 'expert'), may hold values from 1e-10 to 1e-08
- live_block_count: int32 [4], replicated, may hold values from 1 to 8, as said below
- holder_table: int32 [4, 8], replicated, may hold values from 0 to 3, as said below
- slot_table: int32 [4, 8], replicated, may hold values from 0 to 7, as said below
- step_count: int32 [1], replicated, may hold values from 1 to 40
Outputs:
- updated_attention: float32 [6144, 1024], P('dp', 'expert')
- updated_means: float32 [6144, 1024], P('dp', 'expert')
- updated_squares: float32 [6144, 1024], P('dp', 'expert')
- updated_experts: float32 [8, 4, 8, 6144], P('dp', 'expert')
- expert_means: float32 [8, 4, 8, 6144], P('dp', 'expert')
- expert_squares: float32 [8, 4, 8, 6144], P('dp', 'expert')
The draws below stay inside these ranges and needn't reach their ends.
Inputs may be any that keep to these rules, and one draw needn't show every extreme that they name: `live_block_count`: every expert has 1 to 8 live blocks and some expert has exactly 8. `holder_table`: no holder holds more than 2 live blocks of one expert, and some holder holds exactly 2 of one. `slot_table`: the blocks on one holder sit in distinct slots, and some holder has all 8 slots live.
All inputs are finite; a program needn't handle non-finite values.
Results may differ from the reference program's by a relative error of at most 0.0003.
Values sent between devices are 32-bit elements; how exact they have to be, the bound alone decides.
A program may use at most 64 MiB of HBM per device.

```python
import math
import jax
import jax.numpy as jnp
from jax import lax

D = 6144
KV_COLS = 1024
MAXB = 8
HSLOTS = 8
CAP = 2
N_DP = 8
N_EXPERT = 4


def placement_tables(key):
    base = jax.random.fold_in(key, 7)
    key_order, key_turn, key_count = jax.random.split(base, 3)
    order = jax.random.permutation(key_order, N_EXPERT).astype(jnp.int32)
    turns = jax.random.randint(key_turn, (N_EXPERT,), 0, HSLOTS, dtype=jnp.int32)
    counts = jax.random.randint(key_count, (N_EXPERT,), 1, MAXB + 1, dtype=jnp.int32)
    floor_count = MAXB - order * CAP
    counts = jnp.where(order < MAXB // CAP, jnp.maximum(counts, floor_count), counts)
    block_position = jnp.arange(MAXB, dtype=jnp.int32)
    holders = ((order[:, None] + block_position[None, :] // CAP) % N_EXPERT).astype(jnp.int32)
    slots = ((block_position[None, :] + turns[holders]) % HSLOTS).astype(jnp.int32)
    return (counts.astype(jnp.int32), holders, slots)


def draw_live_block_count(key, part):
    return placement_tables(key)[0]


def draw_holder_table(key, part):
    return placement_tables(key)[1]


def draw_slot_table(key, part):
    return placement_tables(key)[2]


def draw_attention_gradient(key, part):
    key_noise, key_rows, key_cols, key_source = jax.random.split(key, 4)
    noise = jax.random.normal(key_noise, (N_DP, D, KV_COLS), jnp.float32)
    rising = jnp.power(3.0, jnp.arange(D, dtype=jnp.float32) / D)
    row_scale = rising * jnp.exp(jax.random.uniform(key_rows, (D,), jnp.float32, 0.0, math.log(3.4)))
    col_scale = jnp.exp(jax.random.uniform(key_cols, (KV_COLS,), jnp.float32, 0.0, math.log(3.0)))
    source = jnp.exp(jax.random.uniform(key_source, (N_DP, 1, 1), jnp.float32, math.log(0.5), math.log(2.0)))
    return (noise * source * row_scale[None, :, None] * col_scale[None, None, :]).astype(jnp.bfloat16)


def draw_expert_gradient(key, part):
    key_noise, key_blocks, key_cols = jax.random.split(key, 3)
    shape = (N_DP, N_EXPERT, MAXB, D)
    noise = jax.random.normal(key_noise, shape, jnp.float32)
    flat = jnp.arange(N_DP * N_EXPERT, dtype=jnp.float32).reshape(N_DP, N_EXPERT) / (N_DP * N_EXPERT)
    rising = jnp.power(3.0, flat)[:, :, None, None]
    block_scale = jnp.exp(jax.random.uniform(key_blocks, (N_DP, N_EXPERT, MAXB, 1), jnp.float32, 0.0, math.log(10.0)))
    col_scale = jnp.exp(jax.random.uniform(key_cols, (D,), jnp.float32, 0.0, math.log(3.0)))
    return noise * rising * block_scale * col_scale[None, None, None, :]


def levels(rng, dims, cuts, low, high):
    level = 1.0
    for position, blocks in cuts:
        draws = jax.random.uniform(jax.random.fold_in(jax.random.fold_in(rng, 6), position), (blocks,), jnp.float32, low / len(cuts), high / len(cuts))
        level = level * jnp.repeat(jnp.exp(draws), dims[position] // blocks).reshape((-1,) + (1,) * (len(dims) - 1 - position))
    return level


def bell_draw(key, extent, deviation, reach, cuts=(), kind=jnp.bfloat16):
    entries = deviation * jax.random.normal(key, extent, jnp.float32)
    if cuts:
        entries = entries * levels(key, extent, cuts, -0.22, 0.18)
    return jnp.clip(entries, -reach, reach).astype(kind)


def setup_inputs(seed: int = 0) -> dict:
    streams_of = jax.random.split(jax.random.key(seed), 13)
    attention_gradient = draw_attention_gradient(jax.random.fold_in(streams_of[12], 71), 0)
    attention_weight = bell_draw(streams_of[1], (D, KV_COLS), 1.0, 6.0, ((0, 8), (1, 4)), jnp.float32)
    attention_mean = bell_draw(streams_of[2], (D, KV_COLS), 0.0002, 0.0012, ((0, 8), (1, 4)), jnp.float32)
    attention_square = jnp.clip(jnp.exp(math.log(1.0000000116860974e-07) - 4.6051702 * jax.random.uniform(streams_of[3], (D, KV_COLS), jnp.float32) ** levels(streams_of[3], (D, KV_COLS), ((0, 8), (1, 4)), -0.2, 0.2)), 9.999999717180685e-10, 1.0000000116860974e-07)
    expert_gradient = draw_expert_gradient(jax.random.fold_in(streams_of[12], 71), 0)
    expert_weight = bell_draw(streams_of[5], (N_DP, N_EXPERT, MAXB, D), 1.0, 6.0, ((0, 8), (1, 4)), jnp.float32)
    held_mean = bell_draw(streams_of[6], (N_DP, N_EXPERT * HSLOTS, D), 0.0001, 0.0006, ((0, 8), (1, 4)), jnp.float32)
    held_square = jnp.clip(jnp.exp(math.log(9.99999993922529e-09) - 4.6051702 * jax.random.uniform(streams_of[7], (N_DP, N_EXPERT * HSLOTS, D), jnp.float32) ** levels(streams_of[7], (N_DP, N_EXPERT * HSLOTS, D), ((0, 8), (1, 4)), -0.2, 0.2)), 1.000000013351432e-10, 9.99999993922529e-09)
    live_block_count = draw_live_block_count(jax.random.fold_in(streams_of[12], 71), 0)
    holder_table = draw_holder_table(jax.random.fold_in(streams_of[12], 71), 0)
    slot_table = draw_slot_table(jax.random.fold_in(streams_of[12], 71), 0)
    step_count = jax.random.randint(streams_of[11], (1,), 1, 41).astype(jnp.int32)
    return dict(attention_gradient=attention_gradient, attention_weight=attention_weight, attention_mean=attention_mean, attention_square=attention_square, expert_gradient=expert_gradient, expert_weight=expert_weight, held_mean=held_mean, held_square=held_square, live_block_count=live_block_count, holder_table=holder_table, slot_table=slot_table, step_count=step_count)


beta_first = 0.9
beta_second = 0.95
learn_rate = 0.1
decay_rate = 0.1
adam_epsilon = 1e-08
clip_norm = 1.0

def adam_step(weight, mean, square, gradient, factor, step_float):
    scaled = factor * gradient
    mean_new = beta_first * mean + (1.0 - beta_first) * scaled
    square_new = beta_second * square + (1.0 - beta_second) * scaled * scaled
    mean_hat = mean_new / (1.0 - jnp.power(beta_first, step_float))
    square_hat = square_new / (1.0 - jnp.power(beta_second, step_float))
    weight_new = weight - learn_rate * (mean_hat / (jnp.sqrt(square_hat) + adam_epsilon) + decay_rate * weight)
    return (weight_new, mean_new, square_new)

def reference(attention_gradient, attention_weight, attention_mean, attention_square, expert_gradient, expert_weight, held_mean, held_square, live_block_count, holder_table, slot_table, step_count):

    def accumulate(running, piece):
        return (running + piece.astype(jnp.float32), None)
    summed, _ = lax.scan(accumulate, jnp.zeros(attention_gradient.shape[1:], jnp.float32), attention_gradient)
    block_position = jnp.arange(MAXB, dtype=jnp.int32)
    live_block_mask = (block_position[None, :] < live_block_count[:, None]).astype(jnp.float32)
    spread_blocks = live_block_mask[None, :, :, None]
    attention_part = jnp.sum(summed * summed)
    expert_share = jnp.sum(spread_blocks * expert_gradient * expert_gradient)
    total = attention_part + expert_share
    factor = jnp.minimum(1.0, clip_norm / (jnp.sqrt(total) + 1e-06))
    step_float = step_count[0].astype(jnp.float32)
    attention_new, means_new, squares_new = adam_step(attention_weight, attention_mean, attention_square, summed, factor, step_float)
    indices = (holder_table * HSLOTS + slot_table).astype(jnp.int32)
    owned_mean = held_mean[:, indices, :] * spread_blocks
    owned_square = held_square[:, indices, :] * spread_blocks
    weight_next, mean_next, square_next = adam_step(expert_weight, owned_mean, owned_square, expert_gradient, factor, step_float)
    live_flags = spread_blocks > 0.5
    experts_new = jnp.where(live_flags, weight_next, expert_weight)
    expert_means = jnp.where(live_flags, mean_next, 0.0)
    expert_squares = jnp.where(live_flags, square_next, 0.0)
    return (attention_new, means_new, squares_new, experts_new, expert_means, expert_squares)
```

```python
import functools

import jax
import jax.numpy as jnp
from jax import lax
from jax.experimental import pallas as pl
from jax.experimental.pallas import tpu as pltpu
from jax.sharding import PartitionSpec as P

MESH = pl.DeviceIdType.MESH
CORES = 2
LIMIT = 40 * 1024 * 1024

beta_first = 0.9
beta_second = 0.95
learn_rate = 0.1
decay_rate = 0.1
adam_epsilon = 1e-08
clip_norm = 1.0


def power(base, exponent):
    result = jnp.float32(1.0)
    value = base
    for bit in range(31):
        factor = value if value > 1e-37 else 0.0
        result = jnp.where((exponent >> bit) & 1 == 1, result * jnp.float32(factor), result)
        value = value * value
    return result


def far_first(size):
    return sorted(range(size), key=lambda k: (-min(k, size - k), k))


def kernel(
    levels, experts, per_holder, cuts,
    grad_hbm, eg_hbm, ew_hbm, w_hbm, m_hbm, v_hbm, hm_hbm, hs_hbm, count_hbm, holder_hbm, slot_hbm, step_hbm,
    sum_ref, wmv, blocks, scale_ref,
    grad, pair_out, local, recv, held, mom_out, mom_in, part, parts,
    count_ref, holder_ref, slot_ref, step_ref,
    grad_sem, load_sem, pair_send, pair_recv, link_send, link_recv,
    mom_send, mom_recv, part_send, part_recv,
):
    dp = lax.axis_index("dp")
    me = lax.axis_index("expert")
    z = dp // CORES
    core = dp % CORES
    other = 1 - core
    partner = z * CORES + other
    upper = 2 * z >= levels
    maxb = holder_ref.shape[1]
    rows = sum_ref.shape[0]
    steps = len(cuts)
    devices = levels * CORES * experts
    spans = [pl.ds(start, size) for start, size in cuts]

    def level_of(j):
        return jnp.where(upper, j, levels - 1 - j)

    first = level_of(0)
    head = cuts[0][1]

    def load_level(j):
        d = level_of(j)
        return pltpu.make_async_copy(grad_hbm.at[d], grad.at[d], grad_sem.at[j])

    def load_first(i, start, size):
        span = pl.ds(start, size)
        return pltpu.make_async_copy(grad_hbm.at[first, :, span], grad.at[first, :, span], grad_sem.at[i])

    opening = [load_first(0, 0, head)]
    if rows > head:
        opening.append(load_first(levels, head, rows - head))
    opening[0].start()

    barrier = pltpu.get_barrier_semaphore()
    pl.semaphore_signal(barrier, inc=1, device_id=(partner, me), device_id_type=MESH)

    @pl.when(z > 0)
    def _():
        pl.semaphore_signal(barrier, inc=1, device_id=(dp - CORES, me), device_id_type=MESH)

    @pl.when(z < levels - 1)
    def _():
        pl.semaphore_signal(barrier, inc=1, device_id=(dp + CORES, me), device_id_type=MESH)

    for off in range(1, experts):
        pl.semaphore_signal(barrier, inc=1, device_id=(dp, lax.rem(me + off, experts)), device_id_type=MESH)

    for load in opening[1:]:
        load.start()
    for j in range(1, levels):
        load_level(j).start()

    def pair_copy(d, span, sem):
        return pltpu.make_async_remote_copy(
            src_ref=pair_out.at[d, span], dst_ref=local.at[d, span],
            send_sem=pair_send, recv_sem=pair_recv.at[sem],
            device_id=(partner, me), device_id_type=MESH,
        )

    def link_copy(way, d, p, src):
        slot = d + 1 - way
        return pltpu.make_async_remote_copy(
            src_ref=src, dst_ref=recv.at[slot, spans[p]],
            send_sem=link_send, recv_sem=link_recv.at[slot, p],
            device_id=(jnp.where(way == 0, dp + CORES, dp - CORES), me), device_id_type=MESH,
        )

    way_out = jnp.where(upper, 1, 0)
    at_end = (z == 0) | (z == levels - 1)

    opening[0].wait()
    pair_out[first, spans[0]] = grad[first, other, spans[0]].astype(jnp.float32)
    near = jnp.where(z > 0, 1, 0) + jnp.where(z < levels - 1, 1, 0)
    pl.semaphore_wait(barrier, experts + near)
    pair_copy(first, spans[0], 0).start()
    for load in opening[1:]:
        load.wait()
    for p in range(1, steps):
        pair_out[first, spans[p]] = grad[first, other, spans[p]].astype(jnp.float32)
        pair_copy(first, spans[p], p).start()

    for p in range(steps):
        pair_copy(first, spans[p], p).wait_recv()
        local[first, spans[p]] = local[first, spans[p]] + grad[first, core, spans[p]].astype(jnp.float32)

        @pl.when(at_end & (first != z))
        def _():
            link_copy(way_out, first, p, local.at[first, spans[p]]).start()

    whole = pl.ds(0, rows)

    def give(j):
        load_level(j).wait()
        d = level_of(j)
        pair_out[d] = grad[d, other].astype(jnp.float32)
        pair_copy(d, whole, steps + j - 1).start()

    def take(j):
        d = level_of(j)
        pair_copy(d, whole, steps + j - 1).wait_recv()
        local[d] = local[d] + grad[d, core].astype(jnp.float32)

        @pl.when(at_end & (j < levels - 2))
        def _():
            for p in range(steps):
                link_copy(way_out, d, p, local.at[d, spans[p]]).start()

        @pl.when(at_end & (j == levels - 2))
        def _():
            for p in reversed(range(steps)):
                link_copy(way_out, d, p, local.at[d, spans[p]]).start()

    ints = [
        pltpu.make_async_copy(a, b, load_sem.at[i])
        for i, (a, b) in enumerate(((count_hbm, count_ref), (holder_hbm, holder_ref), (slot_hbm, slot_ref), (step_hbm, step_ref)))
    ]
    for load in ints:
        load.start()
    for i, source in enumerate((hm_hbm, hs_hbm)):
        pltpu.make_async_copy(source, held.at[i], load_sem.at[4]).start()

    if levels > 1:
        give(1)

    @pl.loop(1, levels)
    def _(j):
        @pl.when(j + 1 < levels)
        def _():
            give(j + 1)

        take(j)

    for i, source in enumerate((w_hbm, m_hbm, v_hbm)):
        pltpu.make_async_copy(source, wmv.at[i], load_sem.at[5]).start()
    for i, source in enumerate((eg_hbm, ew_hbm)):
        pltpu.make_async_copy(source, blocks.at[i], load_sem.at[6]).start()
    for load in ints:
        load.wait()
    pltpu.make_async_copy(held, held, load_sem.at[4]).wait()

    def moment_copy(target, source):
        return pltpu.make_async_remote_copy(
            src_ref=mom_out.at[target], dst_ref=mom_in.at[source],
            send_sem=mom_send, recv_sem=mom_recv,
            device_id=(dp, target), device_id_type=MESH,
        )

    def picks(owner):
        rank = jnp.int32(0)
        chosen = [jnp.int32(0)] * per_holder
        for b in range(maxb):
            mine = (holder_ref[owner, b] == me) & (b < count_ref[owner])
            for q in range(per_holder):
                chosen[q] = jnp.where(mine & (rank == q), slot_ref[owner, b], chosen[q])
            rank = rank + jnp.where(mine, 1, 0)
        return chosen

    for q, slot in enumerate(picks(me)):
        for i in range(2):
            mom_in[me, i, pl.ds(q, 1), :] = held[i, pl.ds(slot, 1), :]

    @pl.loop(1, experts)
    def _(off):
        owner = lax.rem(me + off, experts)
        for q, slot in enumerate(picks(owner)):
            for i in range(2):
                mom_out[owner, i, pl.ds(q, 1), :] = held[i, pl.ds(slot, 1), :]
        moment_copy(owner, me).start()

    def forward(way, j, p):
        d = jnp.where(way == 0, levels - 1 - j, j)
        ahead = jnp.where(way == 0, (d > z) & (z > 0), (d < z) & (z < levels - 1))
        slot = d + 1 - way

        @pl.when(ahead)
        def _():
            block = recv.at[slot, spans[p]]
            copy = link_copy(way, d, p, block)
            copy.wait_recv()
            recv[slot, spans[p]] = recv[slot, spans[p]] + local[d, spans[p]]
            copy.start()

    @pl.loop(0, levels)
    def _(j):
        for p in range(steps):
            forward(way_out, j, p)
            if p:
                forward(1 - way_out, j, p - 1)
            else:
                @pl.when(j > 0)
                def _():
                    forward(1 - way_out, j - 1, steps - 1)

    forward(1 - way_out, levels - 1, steps - 1)

    if experts > 1:
        others = mom_in.at[pl.ds(0, experts - 1)]
        pltpu.make_async_copy(others, others, mom_recv).wait()
        others = mom_out.at[pl.ds(0, experts - 1)]
        pltpu.make_async_copy(others, others, mom_send).wait()

    owned = count_ref[me]
    for b in range(maxb):
        holder = holder_ref[me, b]
        rank = jnp.int32(0)
        for earlier in range(b):
            rank = rank + jnp.where((holder_ref[me, earlier] == holder) & (earlier < owned), 1, 0)
        rank = jnp.minimum(rank, per_holder - 1)
        for i in range(2):
            blocks[2 + i, pl.ds(b, 1), :] = mom_in[holder, i, pl.ds(rank, 1), :]
    taken = blocks.at[pl.ds(0, 2)]
    pltpu.make_async_copy(taken, taken, load_sem.at[6]).wait()
    width = blocks.shape[2]
    live = lax.broadcasted_iota(jnp.int32, (maxb, 128), 0) < owned
    acc = jnp.zeros((maxb, 128), jnp.float32)
    for i in range(width // 128):
        span = pl.ds(i * 128, 128)
        g = jnp.where(live, blocks[0, :, span], 0.0)
        w = blocks[1, :, span]
        blocks[0, :, span] = g
        blocks[1, :, span] = jnp.where(live, (1.0 - learn_rate * decay_rate) * w, w)
        blocks[2, :, span] = jnp.where(live, beta_first * blocks[2, :, span], 0.0)
        blocks[3, :, span] = jnp.where(live, beta_second * blocks[3, :, span], 0.0)
        acc = acc + g * g
    row = jnp.sum(acc, axis=0, keepdims=True)
    pltpu.make_async_copy(wmv, wmv, load_sem.at[5]).wait()
    for i, scale in enumerate((1.0 - learn_rate * decay_rate, beta_first, beta_second)):
        wmv[i] = wmv[i] * scale
    step = step_ref[0]
    one = jnp.ones((1, 128), jnp.float32)
    first_left = one * (1.0 - power(beta_first, step))
    second_root = jnp.sqrt(one * (1.0 - power(beta_second, step)))
    scale_ref[2:3] = learn_rate * second_root / first_left
    scale_ref[3:4] = adam_epsilon * second_root

    early = 1 - way_out
    inner = jnp.where(upper, z > 0, z < levels - 1)
    outer = jnp.where(upper, z < levels - 1, z > 0)
    for p in range(steps):
        @pl.when(inner)
        def _():
            link_copy(early, z, p, recv.at[z + 1 - early, spans[p]]).wait_recv()
            sum_ref[spans[p]] = local[z, spans[p]] + recv[z + 1 - early, spans[p]]

        @pl.when(jnp.logical_not(inner))
        def _():
            sum_ref[spans[p]] = local[z, spans[p]]

    for p in reversed(range(steps)):
        @pl.when(outer)
        def _():
            link_copy(way_out, z, p, recv.at[z + 1 - way_out, spans[p]]).wait_recv()
            sum_ref[spans[p]] = sum_ref[spans[p]] + recv[z + 1 - way_out, spans[p]]

        g = sum_ref[spans[p]]
        col = jnp.sum(g * g, axis=0, keepdims=True)
        for i in range(g.shape[1] // 128):
            row = row + col[:, i * 128:(i + 1) * 128]

    index = dp * experts + me
    part[...] = row
    parts[index] = row

    def part_copy(target_dp, target_me):
        return pltpu.make_async_remote_copy(
            src_ref=part, dst_ref=parts.at[index],
            send_sem=part_send, recv_sem=part_recv,
            device_id=(target_dp, target_me), device_id_type=MESH,
        )

    if devices <= 64:
        for far in far_first(levels):
            side = lax.rem(z + far, levels) * CORES
            for off in far_first(experts):
                target = lax.rem(me + off, experts)
                for swap in range(CORES):
                    if far or off or swap:
                        part_copy(side + lax.rem(core + swap, CORES), target).start()
    else:
        @pl.loop(1, devices)
        def _(off):
            target = lax.rem(index + off, devices)
            part_copy(target // experts, lax.rem(target, experts)).start()

    pltpu.make_async_copy(pair_out, pair_out, pair_send).wait()
    if levels > 1:
        sent = local.at[pl.ds(0, levels - 1)]
        pltpu.make_async_copy(sent, sent, link_send).wait()
    others = parts.at[pl.ds(0, devices - 1)]
    pltpu.make_async_copy(others, others, part_send).wait()
    pltpu.make_async_copy(others, others, part_recv).wait()
    total = jnp.sum(jnp.sum(parts[...], axis=0), axis=1, keepdims=True)
    factor = jnp.broadcast_to(jnp.minimum(1.0, clip_norm / (jnp.sqrt(total) + 1e-06)), (1, 128))
    scale_ref[0:1] = (1.0 - beta_first) * factor
    scale_ref[1:2] = (1.0 - beta_second) ** 0.5 * factor


def update(
    wmv, sums, blocks, scale_ref,
    ow_hbm, om_hbm, ov_hbm, oew_hbm, oem_hbm, oes_hbm,
    out, block_out, sem, block_sem,
):
    first_factor = scale_ref[0:1, 0:1]
    second_factor = scale_ref[1:2, 0:1]
    rate = scale_ref[2:3, 0:1]
    epsilon = scale_ref[3:4, 0:1]
    rows = sums.shape[0]
    size = chunk_rows(rows)

    @pl.loop(0, rows // size)
    def _(c):
        span = pl.ds(pl.multiple_of(c * size, size), size)
        g = sums[span]
        m = wmv[1, span] + first_factor * g
        s = second_factor * g
        v = wmv[2, span] + s * s
        out[1, span] = m
        out[2, span] = v
        out[0, span] = wmv[0, span] - rate * m / (v * lax.rsqrt(v) + epsilon)
        for i, dst in enumerate((ow_hbm, om_hbm, ov_hbm)):
            pltpu.make_async_copy(out.at[i, span], dst.at[span], sem).start()

    width = blocks.shape[2]
    for i in range(width // 128):
        cols = pl.ds(i * 128, 128)
        g = blocks[0, :, cols]
        m = blocks[2, :, cols] + first_factor * g
        s = second_factor * g
        v = blocks[3, :, cols] + s * s
        block_out[1, :, cols] = m
        block_out[2, :, cols] = v
        block_out[0, :, cols] = blocks[1, :, cols] - rate * m / (jnp.sqrt(v) + epsilon)
    for i, dst in enumerate((oew_hbm, oem_hbm, oes_hbm)):
        pltpu.make_async_copy(block_out.at[i], dst, block_sem).start()
    pltpu.make_async_copy(out, out, sem).wait()
    pltpu.make_async_copy(block_out, block_out, block_sem).wait()


def chunk_rows(rows):
    for size in range(96, 0, -8):
        if rows % size == 0:
            return size
    return rows


def cut_rows(rows):
    if rows % 16:
        return ((0, rows),)
    head = max(16, rows // 12 // 16 * 16)
    half = (rows - head) // 2 // 16 * 16
    sizes = [size for size in (head, half, rows - head - half) if size > 0]
    starts = [sum(sizes[:i]) for i in range(len(sizes))]
    return tuple(zip(starts, sizes))


def make_body(mesh):
    n_dp = mesh.shape["dp"]
    experts = mesh.shape["expert"]
    levels = n_dp // CORES

    def body(ag, aw, am, av, eg, ew, hm, hs, count, holder, slot, step):
        depth, cols = ag.shape[1], ag.shape[2]
        rows = depth // n_dp
        cuts = cut_rows(rows)
        maxb, width = eg.shape[2], eg.shape[3]
        slots = hm.shape[1]
        per_holder = max(1, maxb // experts)
        f32 = jnp.float32
        dma = pltpu.SemaphoreType.DMA
        hbm = pl.BlockSpec(memory_space=pltpu.HBM)
        vmem = pl.BlockSpec(memory_space=pltpu.VMEM)
        shape = jax.ShapeDtypeStruct
        moved = (experts, 2, per_holder, width)
        sums, wmv, blocks, scales = pl.pallas_call(
            functools.partial(kernel, levels, experts, per_holder, cuts),
            out_shape=[pltpu.VMEM(s, f32) for s in ((rows, cols), (3, rows, cols), (4, maxb, width), (4, 128))],
            in_specs=[hbm] * 12,
            out_specs=[vmem] * 4,
            scratch_shapes=[
                pltpu.VMEM((levels, CORES, rows, cols), ag.dtype),
                pltpu.VMEM((levels, rows, cols), f32),
                pltpu.VMEM((levels, rows, cols), f32),
                pltpu.VMEM((levels + 1, rows, cols), f32),
                pltpu.VMEM((2, slots, width), f32),
                pltpu.VMEM(moved, f32), pltpu.VMEM(moved, f32),
                pltpu.VMEM((1, 128), f32), pltpu.VMEM((n_dp * experts, 1, 128), f32),
                pltpu.SMEM(count.shape, jnp.int32), pltpu.SMEM(holder.shape, jnp.int32),
                pltpu.SMEM(slot.shape, jnp.int32), pltpu.SMEM(step.shape, jnp.int32),
                dma((levels + 1,)), dma((7,)), dma(()), dma((len(cuts) + levels - 1,)),
                dma(()), dma((levels + 1, len(cuts))),
                dma(()), dma(()), dma(()), dma(()),
            ],
            compiler_params=pltpu.CompilerParams(
                collective_id=0, has_side_effects=True, vmem_limit_bytes=LIMIT
            ),
        )(
            *(pltpu.with_memory_space_constraint(x, pltpu.HBM) for x in (
                ag.reshape(levels, CORES, rows, cols), eg[0, 0], ew[0, 0],
                aw, am, av, hm[0], hs[0], count, holder, slot,
            )),
            step,
        )
        outs = pl.pallas_call(
            update,
            out_shape=[shape((rows, cols), f32)] * 3 + [shape((maxb, width), f32)] * 3,
            in_specs=[vmem] * 4,
            out_specs=[hbm] * 6,
            scratch_shapes=[pltpu.VMEM((3, rows, cols), f32), pltpu.VMEM((3, maxb, width), f32), dma(()), dma(())],
            compiler_params=pltpu.CompilerParams(vmem_limit_bytes=16 * 1024 * 1024),
        )(wmv, sums, blocks, scales)
        return tuple(outs[:3]) + tuple(o[None, None] for o in outs[3:])

    return body


def solution(mesh):
    matrix = P("dp", "expert")
    blocks = P("dp", "expert", None, None)
    held = P("dp", "expert", None)
    return jax.shard_map(
        make_body(mesh),
        mesh=mesh,
        in_specs=(P("dp", None, "expert"), matrix, matrix, matrix, blocks, blocks, held, held, P(), P(), P(), P()),
        out_specs=(matrix, matrix, matrix, blocks, blocks, blocks),
        check_vma=False,
    )
```

```python
import functools

import jax
import jax.numpy as jnp
from jax import lax
from jax.experimental import pallas as pl
from jax.experimental.pallas import tpu as pltpu
from jax.sharding import PartitionSpec as P

MESH = pl.DeviceIdType.MESH
CORES = 2
LIMIT = 40 * 1024 * 1024

beta_first = 0.9
beta_second = 0.95
learn_rate = 0.1
decay_rate = 0.1
adam_epsilon = 1e-08
clip_norm = 1.0


def power(base, exponent):
    result = jnp.float32(1.0)
    value = base
    for bit in range(31):
        factor = value if value > 1e-37 else 0.0
        result = jnp.where((exponent >> bit) & 1 == 1, result * jnp.float32(factor), result)
        value = value * value
    return result


def far_first(size):
    return sorted(range(size), key=lambda k: (-min(k, size - k), k))


def kernel(
    levels, experts, per_holder, cuts,
    grad_hbm, eg_hbm, ew_hbm, w_hbm, m_hbm, v_hbm, hm_hbm, hs_hbm, count_hbm, holder_hbm, slot_hbm, step_hbm,
    sum_ref, wmv, blocks, scale_ref,
    grad, pair_out, local, recv, held, mom_out, mom_in, part, parts,
    count_ref, holder_ref, slot_ref, step_ref,
):
    dma = pltpu.SemaphoreType.DMA
    pl.run_scoped(
        functools.partial(
            scoped, levels, experts, per_holder, cuts,
            grad_hbm, eg_hbm, ew_hbm, w_hbm, m_hbm, v_hbm, hm_hbm, hs_hbm, count_hbm, holder_hbm, slot_hbm, step_hbm,
            sum_ref, wmv, blocks, scale_ref,
            grad, pair_out, local, recv, held, mom_out, mom_in, part, parts,
            count_ref, holder_ref, slot_ref, step_ref,
        ),
        dma((levels + 1,)), dma((7,)), dma(()), dma((len(cuts) + levels - 1,)),
        dma(()), dma((levels + 1, len(cuts))),
        dma(()), dma(()), dma(()), dma(()),
    )


def scoped(
    levels, experts, per_holder, cuts,
    grad_hbm, eg_hbm, ew_hbm, w_hbm, m_hbm, v_hbm, hm_hbm, hs_hbm, count_hbm, holder_hbm, slot_hbm, step_hbm,
    sum_ref, wmv, blocks, scale_ref,
    grad, pair_out, local, recv, held, mom_out, mom_in, part, parts,
    count_ref, holder_ref, slot_ref, step_ref,
    grad_sem, load_sem, pair_send, pair_recv, link_send, link_recv,
    mom_send, mom_recv, part_send, part_recv,
):
    dp = lax.axis_index("dp")
    me = lax.axis_index("expert")
    z = dp // CORES
    core = dp % CORES
    other = 1 - core
    partner = z * CORES + other
    upper = 2 * z >= levels
    maxb = holder_ref.shape[1]
    rows = sum_ref.shape[0]
    steps = len(cuts)
    devices = levels * CORES * experts
    spans = [pl.ds(start, size) for start, size in cuts]

    def level_of(j):
        return jnp.where(upper, j, levels - 1 - j)

    first = level_of(0)
    head = cuts[0][1]

    def load_level(j):
        d = level_of(j)
        return pltpu.make_async_copy(grad_hbm.at[d], grad.at[d], grad_sem.at[j])

    def load_first(i, start, size):
        span = pl.ds(start, size)
        return pltpu.make_async_copy(grad_hbm.at[first, :, span], grad.at[first, :, span], grad_sem.at[i])

    opening = [load_first(0, 0, head)]
    if rows > head:
        opening.append(load_first(levels, head, rows - head))
    opening[0].start()

    barrier = pltpu.get_barrier_semaphore()
    pl.semaphore_signal(barrier, inc=1, device_id=(partner, me), device_id_type=MESH)

    @pl.when(z > 0)
    def _():
        pl.semaphore_signal(barrier, inc=1, device_id=(dp - CORES, me), device_id_type=MESH)

    @pl.when(z < levels - 1)
    def _():
        pl.semaphore_signal(barrier, inc=1, device_id=(dp + CORES, me), device_id_type=MESH)

    for off in range(1, experts):
        pl.semaphore_signal(barrier, inc=1, device_id=(dp, lax.rem(me + off, experts)), device_id_type=MESH)

    for load in opening[1:]:
        load.start()
    for j in range(1, levels):
        load_level(j).start()

    def pair_copy(d, span, sem):
        return pltpu.make_async_remote_copy(
            src_ref=pair_out.at[d, span], dst_ref=local.at[d, span],
            send_sem=pair_send, recv_sem=pair_recv.at[sem],
            device_id=(partner, me), device_id_type=MESH,
        )

    def link_copy(way, d, p, src):
        slot = d + 1 - way
        return pltpu.make_async_remote_copy(
            src_ref=src, dst_ref=recv.at[slot, spans[p]],
            send_sem=link_send, recv_sem=link_recv.at[slot, p],
            device_id=(jnp.where(way == 0, dp + CORES, dp - CORES), me), device_id_type=MESH,
        )

    way_out = jnp.where(upper, 1, 0)
    at_end = (z == 0) | (z == levels - 1)

    opening[0].wait()
    pair_out[first, spans[0]] = grad[first, other, spans[0]].astype(jnp.float32)
    near = jnp.where(z > 0, 1, 0) + jnp.where(z < levels - 1, 1, 0)
    pl.semaphore_wait(barrier, experts + near)
    pair_copy(first, spans[0], 0).start()
    for load in opening[1:]:
        load.wait()
    for p in range(1, steps):
        pair_out[first, spans[p]] = grad[first, other, spans[p]].astype(jnp.float32)
        pair_copy(first, spans[p], p).start()

    for p in range(steps):
        pair_copy(first, spans[p], p).wait_recv()
        local[first, spans[p]] = local[first, spans[p]] + grad[first, core, spans[p]].astype(jnp.float32)

        @pl.when(at_end & (first != z))
        def _():
            link_copy(way_out, first, p, local.at[first, spans[p]]).start()

    whole = pl.ds(0, rows)

    def give(j):
        load_level(j).wait()
        d = level_of(j)
        pair_out[d] = grad[d, other].astype(jnp.float32)
        pair_copy(d, whole, steps + j - 1).start()

    def take(j):
        d = level_of(j)
        pair_copy(d, whole, steps + j - 1).wait_recv()
        local[d] = local[d] + grad[d, core].astype(jnp.float32)

        @pl.when(at_end & (j < levels - 2))
        def _():
            for p in range(steps):
                link_copy(way_out, d, p, local.at[d, spans[p]]).start()

        @pl.when(at_end & (j == levels - 2))
        def _():
            for p in reversed(range(steps)):
                link_copy(way_out, d, p, local.at[d, spans[p]]).start()

    ints = [
        pltpu.make_async_copy(a, b, load_sem.at[i])
        for i, (a, b) in enumerate(((count_hbm, count_ref), (holder_hbm, holder_ref), (slot_hbm, slot_ref), (step_hbm, step_ref)))
    ]
    for load in ints:
        load.start()
    for i, source in enumerate((hm_hbm, hs_hbm)):
        pltpu.make_async_copy(source, held.at[i], load_sem.at[4]).start()

    if levels > 1:
        give(1)

    @pl.loop(1, levels)
    def _(j):
        @pl.when(j + 1 < levels)
        def _():
            give(j + 1)

        take(j)

    for i, source in enumerate((w_hbm, m_hbm, v_hbm)):
        pltpu.make_async_copy(source, wmv.at[i], load_sem.at[5]).start()
    for i, source in enumerate((eg_hbm, ew_hbm)):
        pltpu.make_async_copy(source, blocks.at[i], load_sem.at[6]).start()
    for load in ints:
        load.wait()
    pltpu.make_async_copy(held, held, load_sem.at[4]).wait()

    def moment_copy(target, source):
        return pltpu.make_async_remote_copy(
            src_ref=mom_out.at[target], dst_ref=mom_in.at[source],
            send_sem=mom_send, recv_sem=mom_recv,
            device_id=(dp, target), device_id_type=MESH,
        )

    def picks(owner):
        rank = jnp.int32(0)
        chosen = [jnp.int32(0)] * per_holder
        for b in range(maxb):
            mine = (holder_ref[owner, b] == me) & (b < count_ref[owner])
            for q in range(per_holder):
                chosen[q] = jnp.where(mine & (rank == q), slot_ref[owner, b], chosen[q])
            rank = rank + jnp.where(mine, 1, 0)
        return chosen

    for q, slot in enumerate(picks(me)):
        for i in range(2):
            mom_in[me, i, pl.ds(q, 1), :] = held[i, pl.ds(slot, 1), :]

    @pl.loop(1, experts)
    def _(off):
        owner = lax.rem(me + off, experts)
        for q, slot in enumerate(picks(owner)):
            for i in range(2):
                mom_out[owner, i, pl.ds(q, 1), :] = held[i, pl.ds(slot, 1), :]
        moment_copy(owner, me).start()

    def forward(way, j, p):
        d = jnp.where(way == 0, levels - 1 - j, j)
        ahead = jnp.where(way == 0, (d > z) & (z > 0), (d < z) & (z < levels - 1))
        slot = d + 1 - way

        @pl.when(ahead)
        def _():
            block = recv.at[slot, spans[p]]
            copy = link_copy(way, d, p, block)
            copy.wait_recv()
            recv[slot, spans[p]] = recv[slot, spans[p]] + local[d, spans[p]]
            copy.start()

    @pl.loop(0, levels)
    def _(j):
        for p in range(steps):
            forward(way_out, j, p)
            if p:
                forward(1 - way_out, j, p - 1)
            else:
                @pl.when(j > 0)
                def _():
                    forward(1 - way_out, j - 1, steps - 1)

    forward(1 - way_out, levels - 1, steps - 1)

    if experts > 1:
        others = mom_in.at[pl.ds(0, experts - 1)]
        pltpu.make_async_copy(others, others, mom_recv).wait()
        others = mom_out.at[pl.ds(0, experts - 1)]
        pltpu.make_async_copy(others, others, mom_send).wait()

    owned = count_ref[me]
    for b in range(maxb):
        holder = holder_ref[me, b]
        rank = jnp.int32(0)
        for earlier in range(b):
            rank = rank + jnp.where((holder_ref[me, earlier] == holder) & (earlier < owned), 1, 0)
        rank = jnp.minimum(rank, per_holder - 1)
        for i in range(2):
            blocks[2 + i, pl.ds(b, 1), :] = mom_in[holder, i, pl.ds(rank, 1), :]
    taken = blocks.at[pl.ds(0, 2)]
    pltpu.make_async_copy(taken, taken, load_sem.at[6]).wait()
    width = blocks.shape[2]
    live = lax.broadcasted_iota(jnp.int32, (maxb, 128), 0) < owned
    acc = jnp.zeros((maxb, 128), jnp.float32)
    for i in range(width // 128):
        span = pl.ds(i * 128, 128)
        g = jnp.where(live, blocks[0, :, span], 0.0)
        w = blocks[1, :, span]
        blocks[0, :, span] = g
        blocks[1, :, span] = jnp.where(live, (1.0 - learn_rate * decay_rate) * w, w)
        blocks[2, :, span] = jnp.where(live, beta_first * blocks[2, :, span], 0.0)
        blocks[3, :, span] = jnp.where(live, beta_second * blocks[3, :, span], 0.0)
        acc = acc + g * g
    row = jnp.sum(acc, axis=0, keepdims=True)
    pltpu.make_async_copy(wmv, wmv, load_sem.at[5]).wait()
    for i, scale in enumerate((1.0 - learn_rate * decay_rate, beta_first, beta_second)):
        wmv[i] = wmv[i] * scale
    step = step_ref[0]
    one = jnp.ones((1, 128), jnp.float32)
    first_left = one * (1.0 - power(beta_first, step))
    second_root = jnp.sqrt(one * (1.0 - power(beta_second, step)))
    scale_ref[2:3] = learn_rate * second_root / first_left
    scale_ref[3:4] = adam_epsilon * second_root

    early = 1 - way_out
    inner = jnp.where(upper, z > 0, z < levels - 1)
    outer = jnp.where(upper, z < levels - 1, z > 0)
    for p in range(steps):
        @pl.when(inner)
        def _():
            link_copy(early, z, p, recv.at[z + 1 - early, spans[p]]).wait_recv()
            sum_ref[spans[p]] = local[z, spans[p]] + recv[z + 1 - early, spans[p]]

        @pl.when(jnp.logical_not(inner))
        def _():
            sum_ref[spans[p]] = local[z, spans[p]]

    for p in reversed(range(steps)):
        @pl.when(outer)
        def _():
            link_copy(way_out, z, p, recv.at[z + 1 - way_out, spans[p]]).wait_recv()
            sum_ref[spans[p]] = sum_ref[spans[p]] + recv[z + 1 - way_out, spans[p]]

        g = sum_ref[spans[p]]
        col = jnp.sum(g * g, axis=0, keepdims=True)
        for i in range(g.shape[1] // 128):
            row = row + col[:, i * 128:(i + 1) * 128]

    index = dp * experts + me
    part[...] = row
    parts[index] = row

    def part_copy(target_dp, target_me):
        return pltpu.make_async_remote_copy(
            src_ref=part, dst_ref=parts.at[index],
            send_sem=part_send, recv_sem=part_recv,
            device_id=(target_dp, target_me), device_id_type=MESH,
        )

    if devices <= 64:
        for far in far_first(levels):
            side = lax.rem(z + far, levels) * CORES
            for off in far_first(experts):
                target = lax.rem(me + off, experts)
                for swap in range(CORES):
                    if far or off or swap:
                        part_copy(side + lax.rem(core + swap, CORES), target).start()
    else:
        @pl.loop(1, devices)
        def _(off):
            target = lax.rem(index + off, devices)
            part_copy(target // experts, lax.rem(target, experts)).start()

    pltpu.make_async_copy(pair_out, pair_out, pair_send).wait()
    if levels > 1:
        sent = local.at[pl.ds(0, levels - 1)]
        pltpu.make_async_copy(sent, sent, link_send).wait()
    others = parts.at[pl.ds(0, devices - 1)]
    pltpu.make_async_copy(others, others, part_send).wait()
    pltpu.make_async_copy(others, others, part_recv).wait()
    total = jnp.sum(jnp.sum(parts[...], axis=0), axis=1, keepdims=True)
    factor = jnp.broadcast_to(jnp.minimum(1.0, clip_norm / (jnp.sqrt(total) + 1e-06)), (1, 128))
    scale_ref[0:1] = (1.0 - beta_first) * factor
    scale_ref[1:2] = (1.0 - beta_second) ** 0.5 * factor


def update(
    wmv, sums, blocks, scale_ref,
    ow_hbm, om_hbm, ov_hbm, oew_hbm, oem_hbm, oes_hbm,
    out, block_out, sem, block_sem,
):
    first_factor = scale_ref[0:1, 0:1]
    second_factor = scale_ref[1:2, 0:1]
    rate = scale_ref[2:3, 0:1]
    epsilon = scale_ref[3:4, 0:1]
    rows = sums.shape[0]
    size = chunk_rows(rows)

    @pl.loop(0, rows // size)
    def _(c):
        span = pl.ds(pl.multiple_of(c * size, size), size)
        g = sums[span]
        m = wmv[1, span] + first_factor * g
        s = second_factor * g
        v = wmv[2, span] + s * s
        out[1, span] = m
        out[2, span] = v
        out[0, span] = wmv[0, span] - rate * m / (v * lax.rsqrt(v) + epsilon)
        for i, dst in enumerate((ow_hbm, om_hbm, ov_hbm)):
            pltpu.make_async_copy(out.at[i, span], dst.at[span], sem).start()

    width = blocks.shape[2]
    for i in range(width // 128):
        cols = pl.ds(i * 128, 128)
        g = blocks[0, :, cols]
        m = blocks[2, :, cols] + first_factor * g
        s = second_factor * g
        v = blocks[3, :, cols] + s * s
        block_out[1, :, cols] = m
        block_out[2, :, cols] = v
        block_out[0, :, cols] = blocks[1, :, cols] - rate * m / (jnp.sqrt(v) + epsilon)
    for i, dst in enumerate((oew_hbm, oem_hbm, oes_hbm)):
        pltpu.make_async_copy(block_out.at[i], dst, block_sem).start()
    pltpu.make_async_copy(out, out, sem).wait()
    pltpu.make_async_copy(block_out, block_out, block_sem).wait()


def chunk_rows(rows):
    for size in range(96, 0, -8):
        if rows % size == 0:
            return size
    return rows


def cut_rows(rows):
    if rows % 16:
        return ((0, rows),)
    head = max(16, rows // 12 // 16 * 16)
    half = (rows - head) // 2 // 16 * 16
    sizes = [size for size in (head, half, rows - head - half) if size > 0]
    starts = [sum(sizes[:i]) for i in range(len(sizes))]
    return tuple(zip(starts, sizes))


def make_body(mesh):
    n_dp = mesh.shape["dp"]
    experts = mesh.shape["expert"]
    levels = n_dp // CORES

    def body(ag, aw, am, av, eg, ew, hm, hs, count, holder, slot, step):
        depth, cols = ag.shape[1], ag.shape[2]
        rows = depth // n_dp
        cuts = cut_rows(rows)
        maxb, width = eg.shape[2], eg.shape[3]
        slots = hm.shape[1]
        per_holder = max(1, maxb // experts)
        f32 = jnp.float32
        hbm = pl.BlockSpec(memory_space=pltpu.HBM)
        vmem = pl.BlockSpec(memory_space=pltpu.VMEM)
        shape = jax.ShapeDtypeStruct
        moved = (experts, 2, per_holder, width)
        sums, wmv, blocks, scales = pl.pallas_call(
            functools.partial(kernel, levels, experts, per_holder, cuts),
            out_shape=[pltpu.VMEM(s, f32) for s in ((rows, cols), (3, rows, cols), (4, maxb, width), (4, 128))],
            in_specs=[hbm] * 12,
            out_specs=[vmem] * 4,
            scratch_shapes=[
                pltpu.VMEM((levels, CORES, rows, cols), ag.dtype),
                pltpu.VMEM((levels, rows, cols), f32),
                pltpu.VMEM((levels, rows, cols), f32),
                pltpu.VMEM((levels + 1, rows, cols), f32),
                pltpu.VMEM((2, slots, width), f32),
                pltpu.VMEM(moved, f32), pltpu.VMEM(moved, f32),
                pltpu.VMEM((1, 128), f32), pltpu.VMEM((n_dp * experts, 1, 128), f32),
                pltpu.SMEM(count.shape, jnp.int32), pltpu.SMEM(holder.shape, jnp.int32),
                pltpu.SMEM(slot.shape, jnp.int32), pltpu.SMEM(step.shape, jnp.int32),
            ],
            compiler_params=pltpu.CompilerParams(
                collective_id=0, has_side_effects=True, vmem_limit_bytes=LIMIT
            ),
        )(
            *(pltpu.with_memory_space_constraint(x, pltpu.HBM) for x in (
                ag.reshape(levels, CORES, rows, cols), eg[0, 0], ew[0, 0],
                aw, am, av, hm[0], hs[0], count, holder, slot,
            )),
            step,
        )
        outs = pl.pallas_call(
            update,
            out_shape=[shape((rows, cols), f32)] * 3 + [shape((maxb, width), f32)] * 3,
            in_specs=[vmem] * 4,
            out_specs=[hbm] * 6,
            scratch_shapes=[pltpu.VMEM((3, rows, cols), f32), pltpu.VMEM((3, maxb, width), f32), pltpu.SemaphoreType.DMA(()), pltpu.SemaphoreType.DMA(())],
            compiler_params=pltpu.CompilerParams(vmem_limit_bytes=16 * 1024 * 1024),
        )(wmv, sums, blocks, scales)
        return tuple(outs[:3]) + tuple(o[None, None] for o in outs[3:])

    return body


def solution(mesh):
    matrix = P("dp", "expert")
    blocks = P("dp", "expert", None, None)
    held = P("dp", "expert", None)
    return jax.shard_map(
        make_body(mesh),
        mesh=mesh,
        in_specs=(P("dp", None, "expert"), matrix, matrix, matrix, blocks, blocks, held, held, P(), P(), P(), P()),
        out_specs=(matrix, matrix, matrix, blocks, blocks, blocks),
        check_vma=False,
    )
```

```python
import functools

import jax
import jax.numpy as jnp
from jax import lax
from jax.experimental import pallas as pl
from jax.experimental.pallas import tpu as pltpu
from jax.sharding import PartitionSpec as P

MESH = pl.DeviceIdType.MESH
CORES = 2
LIMIT = 40 * 1024 * 1024

beta_first = 0.9
beta_second = 0.95
learn_rate = 0.1
decay_rate = 0.1
adam_epsilon = 1e-08
clip_norm = 1.0


def power(base, exponent):
    result = jnp.float32(1.0)
    value = base
    for bit in range(31):
        factor = value if value > 1e-37 else 0.0
        result = jnp.where((exponent >> bit) & 1 == 1, result * jnp.float32(factor), result)
        value = value * value
    return result


def far_first(size):
    return sorted(range(size), key=lambda k: (-min(k, size - k), k))


def kernel(
    levels, experts, per_holder, cuts,
    grad_hbm, eg_hbm, ew_hbm, w_hbm, m_hbm, v_hbm, hm_hbm, hs_hbm, count_hbm, holder_hbm, slot_hbm, step_hbm,
    sum_ref, wmv, blocks, scale_ref,
    grad, pair_out, local, recv, held, mom_out, mom_in, part, parts,
    count_ref, holder_ref, slot_ref, step_ref,
):
    dma = pltpu.SemaphoreType.DMA
    pl.run_scoped(
        functools.partial(
            scoped, levels, experts, per_holder, cuts,
            grad_hbm, eg_hbm, ew_hbm, w_hbm, m_hbm, v_hbm, hm_hbm, hs_hbm, count_hbm, holder_hbm, slot_hbm, step_hbm,
            sum_ref, wmv, blocks, scale_ref,
            grad, pair_out, local, recv, held, mom_out, mom_in, part, parts,
            count_ref, holder_ref, slot_ref, step_ref,
        ),
        dma((levels + 1,)), dma((7,)), dma(()), dma((len(cuts) + levels - 1,)),
        dma(()), dma((levels + 1, len(cuts))),
        dma(()), dma(()), dma(()), dma(()),
    )


def scoped(
    levels, experts, per_holder, cuts,
    grad_hbm, eg_hbm, ew_hbm, w_hbm, m_hbm, v_hbm, hm_hbm, hs_hbm, count_hbm, holder_hbm, slot_hbm, step_hbm,
    sum_ref, wmv, blocks, scale_ref,
    grad, pair_out, local, recv, held, mom_out, mom_in, part, parts,
    count_ref, holder_ref, slot_ref, step_ref,
    grad_sem, load_sem, pair_send, pair_recv, link_send, link_recv,
    mom_send, mom_recv, part_send, part_recv,
):
    dp = lax.axis_index("dp")
    me = lax.axis_index("expert")
    z = dp // CORES
    core = dp % CORES
    other = 1 - core
    partner = z * CORES + other
    upper = 2 * z >= levels
    maxb = holder_ref.shape[1]
    rows = sum_ref.shape[0]
    steps = len(cuts)
    devices = levels * CORES * experts
    spans = [pl.ds(start, size) for start, size in cuts]

    def level_of(j):
        return jnp.where(upper, j, levels - 1 - j)

    first = level_of(0)
    head = cuts[0][1]

    def load_level(j):
        d = level_of(j)
        return pltpu.make_async_copy(grad_hbm.at[d], grad.at[d], grad_sem.at[j])

    def load_first(i, start, size):
        span = pl.ds(start, size)
        return pltpu.make_async_copy(grad_hbm.at[first, :, span], grad.at[first, :, span], grad_sem.at[i])

    opening = [load_first(0, 0, head)]
    if rows > head:
        opening.append(load_first(levels, head, rows - head))
    opening[0].start()

    barrier = pltpu.get_barrier_semaphore()
    pl.semaphore_signal(barrier, inc=1, device_id=(partner, me), device_id_type=MESH)

    @pl.when(z > 0)
    def _():
        pl.semaphore_signal(barrier, inc=1, device_id=(dp - CORES, me), device_id_type=MESH)

    @pl.when(z < levels - 1)
    def _():
        pl.semaphore_signal(barrier, inc=1, device_id=(dp + CORES, me), device_id_type=MESH)

    for off in range(1, experts):
        pl.semaphore_signal(barrier, inc=1, device_id=(dp, lax.rem(me + off, experts)), device_id_type=MESH)

    for load in opening[1:]:
        load.start()
    for j in range(1, levels):
        load_level(j).start()

    def pair_copy(d, span, sem):
        return pltpu.make_async_remote_copy(
            src_ref=pair_out.at[d, span], dst_ref=local.at[d, span],
            send_sem=pair_send, recv_sem=pair_recv.at[sem],
            device_id=(partner, me), device_id_type=MESH,
        )

    def link_copy(way, d, p, src):
        slot = d + 1 - way
        return pltpu.make_async_remote_copy(
            src_ref=src, dst_ref=recv.at[slot, spans[p]],
            send_sem=link_send, recv_sem=link_recv.at[slot, p],
            device_id=(jnp.where(way == 0, dp + CORES, dp - CORES), me), device_id_type=MESH,
        )

    way_out = jnp.where(upper, 1, 0)
    at_end = (z == 0) | (z == levels - 1)

    opening[0].wait()
    pair_out[first, spans[0]] = grad[first, other, spans[0]].astype(jnp.float32)
    near = jnp.where(z > 0, 1, 0) + jnp.where(z < levels - 1, 1, 0)
    pl.semaphore_wait(barrier, experts + near)
    pair_copy(first, spans[0], 0).start()
    for load in opening[1:]:
        load.wait()
    for p in range(1, steps):
        pair_out[first, spans[p]] = grad[first, other, spans[p]].astype(jnp.float32)
        pair_copy(first, spans[p], p).start()

    def open_link(p):
        link_copy(way_out, first, p, local.at[first, spans[p]]).start()

    sender = at_end & (first != z)
    late_core = 1
    for p in range(steps):
        pair_copy(first, spans[p], p).wait_recv()
        local[first, spans[p]] = local[first, spans[p]] + grad[first, core, spans[p]].astype(jnp.float32)
        if p == 0 and steps > 1:
            pl.when(sender & (core != late_core))(lambda: open_link(0))
        elif p == 1:
            pl.when(sender & (core == late_core))(lambda: open_link(0))
        if p or steps == 1:
            pl.when(sender)(lambda: open_link(p))

    whole = pl.ds(0, rows)

    def give(j):
        load_level(j).wait()
        d = level_of(j)
        pair_out[d] = grad[d, other].astype(jnp.float32)
        pair_copy(d, whole, steps + j - 1).start()

    def take(j):
        d = level_of(j)
        pair_copy(d, whole, steps + j - 1).wait_recv()
        local[d] = local[d] + grad[d, core].astype(jnp.float32)

        @pl.when(at_end & (j < levels - 2))
        def _():
            for p in range(steps):
                link_copy(way_out, d, p, local.at[d, spans[p]]).start()

        @pl.when(at_end & (j == levels - 2))
        def _():
            for p in reversed(range(steps)):
                link_copy(way_out, d, p, local.at[d, spans[p]]).start()

    ints = [
        pltpu.make_async_copy(a, b, load_sem.at[i])
        for i, (a, b) in enumerate(((count_hbm, count_ref), (holder_hbm, holder_ref), (slot_hbm, slot_ref), (step_hbm, step_ref)))
    ]
    for load in ints:
        load.start()
    for i, source in enumerate((hm_hbm, hs_hbm)):
        pltpu.make_async_copy(source, held.at[i], load_sem.at[4]).start()

    if levels > 1:
        give(1)

    @pl.loop(1, levels)
    def _(j):
        @pl.when(j + 1 < levels)
        def _():
            give(j + 1)

        take(j)

    for i, source in enumerate((w_hbm, m_hbm, v_hbm)):
        pltpu.make_async_copy(source, wmv.at[i], load_sem.at[5]).start()
    for i, source in enumerate((eg_hbm, ew_hbm)):
        pltpu.make_async_copy(source, blocks.at[i], load_sem.at[6]).start()
    for load in ints:
        load.wait()
    pltpu.make_async_copy(held, held, load_sem.at[4]).wait()

    def moment_copy(target, source):
        return pltpu.make_async_remote_copy(
            src_ref=mom_out.at[target], dst_ref=mom_in.at[source],
            send_sem=mom_send, recv_sem=mom_recv,
            device_id=(dp, target), device_id_type=MESH,
        )

    def picks(owner):
        rank = jnp.int32(0)
        chosen = [jnp.int32(0)] * per_holder
        for b in range(maxb):
            mine = (holder_ref[owner, b] == me) & (b < count_ref[owner])
            for q in range(per_holder):
                chosen[q] = jnp.where(mine & (rank == q), slot_ref[owner, b], chosen[q])
            rank = rank + jnp.where(mine, 1, 0)
        return chosen

    for q, slot in enumerate(picks(me)):
        for i in range(2):
            mom_in[me, i, pl.ds(q, 1), :] = held[i, pl.ds(slot, 1), :]

    @pl.loop(1, experts)
    def _(off):
        owner = lax.rem(me + off, experts)
        for q, slot in enumerate(picks(owner)):
            for i in range(2):
                mom_out[owner, i, pl.ds(q, 1), :] = held[i, pl.ds(slot, 1), :]
        moment_copy(owner, me).start()

    def forward(way, j, p):
        d = jnp.where(way == 0, levels - 1 - j, j)
        ahead = jnp.where(way == 0, (d > z) & (z > 0), (d < z) & (z < levels - 1))
        slot = d + 1 - way

        @pl.when(ahead)
        def _():
            block = recv.at[slot, spans[p]]
            copy = link_copy(way, d, p, block)
            copy.wait_recv()
            recv[slot, spans[p]] = recv[slot, spans[p]] + local[d, spans[p]]
            copy.start()

    @pl.loop(0, levels)
    def _(j):
        for p in range(steps):
            forward(way_out, j, p)
            if p:
                forward(1 - way_out, j, p - 1)
            else:
                @pl.when(j > 0)
                def _():
                    forward(1 - way_out, j - 1, steps - 1)

    forward(1 - way_out, levels - 1, steps - 1)

    if experts > 1:
        others = mom_in.at[pl.ds(0, experts - 1)]
        pltpu.make_async_copy(others, others, mom_recv).wait()
        others = mom_out.at[pl.ds(0, experts - 1)]
        pltpu.make_async_copy(others, others, mom_send).wait()

    owned = count_ref[me]
    for b in range(maxb):
        holder = holder_ref[me, b]
        rank = jnp.int32(0)
        for earlier in range(b):
            rank = rank + jnp.where((holder_ref[me, earlier] == holder) & (earlier < owned), 1, 0)
        rank = jnp.minimum(rank, per_holder - 1)
        for i in range(2):
            blocks[2 + i, pl.ds(b, 1), :] = mom_in[holder, i, pl.ds(rank, 1), :]
    taken = blocks.at[pl.ds(0, 2)]
    pltpu.make_async_copy(taken, taken, load_sem.at[6]).wait()
    width = blocks.shape[2]
    live = lax.broadcasted_iota(jnp.int32, (maxb, 128), 0) < owned
    acc = jnp.zeros((maxb, 128), jnp.float32)
    for i in range(width // 128):
        span = pl.ds(i * 128, 128)
        g = jnp.where(live, blocks[0, :, span], 0.0)
        w = blocks[1, :, span]
        blocks[0, :, span] = g
        blocks[1, :, span] = jnp.where(live, (1.0 - learn_rate * decay_rate) * w, w)
        blocks[2, :, span] = jnp.where(live, beta_first * blocks[2, :, span], 0.0)
        blocks[3, :, span] = jnp.where(live, beta_second * blocks[3, :, span], 0.0)
        acc = acc + g * g
    row = jnp.sum(acc, axis=0, keepdims=True)
    pltpu.make_async_copy(wmv, wmv, load_sem.at[5]).wait()
    for i, scale in enumerate((1.0 - learn_rate * decay_rate, beta_first, beta_second)):
        wmv[i] = wmv[i] * scale
    step = step_ref[0]
    one = jnp.ones((1, 128), jnp.float32)
    first_left = one * (1.0 - power(beta_first, step))
    second_root = jnp.sqrt(one * (1.0 - power(beta_second, step)))
    scale_ref[2:3] = learn_rate * second_root / first_left
    scale_ref[3:4] = adam_epsilon * second_root

    early = 1 - way_out
    inner = jnp.where(upper, z > 0, z < levels - 1)
    outer = jnp.where(upper, z < levels - 1, z > 0)
    for p in range(steps):
        @pl.when(inner)
        def _():
            link_copy(early, z, p, recv.at[z + 1 - early, spans[p]]).wait_recv()
            sum_ref[spans[p]] = local[z, spans[p]] + recv[z + 1 - early, spans[p]]

        @pl.when(jnp.logical_not(inner))
        def _():
            sum_ref[spans[p]] = local[z, spans[p]]

    for p in reversed(range(steps)):
        @pl.when(outer)
        def _():
            link_copy(way_out, z, p, recv.at[z + 1 - way_out, spans[p]]).wait_recv()
            sum_ref[spans[p]] = sum_ref[spans[p]] + recv[z + 1 - way_out, spans[p]]

        g = sum_ref[spans[p]]
        col = jnp.sum(g * g, axis=0, keepdims=True)
        for i in range(g.shape[1] // 128):
            row = row + col[:, i * 128:(i + 1) * 128]

    index = dp * experts + me
    part[...] = row
    parts[index] = row

    def part_copy(target_dp, target_me):
        return pltpu.make_async_remote_copy(
            src_ref=part, dst_ref=parts.at[index],
            send_sem=part_send, recv_sem=part_recv,
            device_id=(target_dp, target_me), device_id_type=MESH,
        )

    if devices <= 64:
        for far in far_first(levels):
            side = lax.rem(z + far, levels) * CORES
            for off in far_first(experts):
                target = lax.rem(me + off, experts)
                for swap in range(CORES):
                    if far or off or swap:
                        part_copy(side + lax.rem(core + swap, CORES), target).start()
    else:
        @pl.loop(1, devices)
        def _(off):
            target = lax.rem(index + off, devices)
            part_copy(target // experts, lax.rem(target, experts)).start()

    pltpu.make_async_copy(pair_out, pair_out, pair_send).wait()
    if levels > 1:
        sent = local.at[pl.ds(0, levels - 1)]
        pltpu.make_async_copy(sent, sent, link_send).wait()
    others = parts.at[pl.ds(0, devices - 1)]
    pltpu.make_async_copy(others, others, part_send).wait()
    pltpu.make_async_copy(others, others, part_recv).wait()
    total = jnp.sum(jnp.sum(parts[...], axis=0), axis=1, keepdims=True)
    factor = jnp.broadcast_to(jnp.minimum(1.0, clip_norm / (jnp.sqrt(total) + 1e-06)), (1, 128))
    scale_ref[0:1] = (1.0 - beta_first) * factor
    scale_ref[1:2] = (1.0 - beta_second) ** 0.5 * factor


def update(
    wmv, sums, blocks, scale_ref,
    ow_hbm, om_hbm, ov_hbm, oew_hbm, oem_hbm, oes_hbm,
    out, block_out, sem, block_sem,
):
    first_factor = scale_ref[0:1, 0:1]
    second_factor = scale_ref[1:2, 0:1]
    rate = scale_ref[2:3, 0:1]
    epsilon = scale_ref[3:4, 0:1]
    def chunk(start, size):
        span = pl.ds(start, size)
        g = sums[span]
        m = wmv[1, span] + first_factor * g
        s = second_factor * g
        v = wmv[2, span] + s * s
        out[1, span] = m
        pltpu.make_async_copy(out.at[1, span], om_hbm.at[span], sem).start()
        out[2, span] = v
        pltpu.make_async_copy(out.at[2, span], ov_hbm.at[span], sem).start()
        out[0, span] = wmv[0, span] - rate * m / (v * lax.rsqrt(v) + epsilon)
        pltpu.make_async_copy(out.at[0, span], ow_hbm.at[span], sem).start()

    rows = sums.shape[0]
    for start, size in chunk_rows(rows):
        chunk(start, size)

    width = blocks.shape[2]
    for i in range(width // 128):
        cols = pl.ds(i * 128, 128)
        g = blocks[0, :, cols]
        m = blocks[2, :, cols] + first_factor * g
        s = second_factor * g
        v = blocks[3, :, cols] + s * s
        block_out[1, :, cols] = m
        block_out[2, :, cols] = v
        block_out[0, :, cols] = blocks[1, :, cols] - rate * m / (jnp.sqrt(v) + epsilon)
    for i, dst in enumerate((oew_hbm, oem_hbm, oes_hbm)):
        pltpu.make_async_copy(block_out.at[i], dst, block_sem).start()
    pltpu.make_async_copy(out, out, sem).wait()
    pltpu.make_async_copy(block_out, block_out, block_sem).wait()


def chunk_rows(rows):
    unit = rows // 8 // 8 * 8
    if not unit or rows % 8:
        return ((0, rows),)
    sizes = [unit, 2 * unit, 2 * unit, rows - 5 * unit]
    return tuple((sum(sizes[:i]), sizes[i]) for i in range(4))


def cut_rows(rows):
    if rows % 16:
        return ((0, rows),)
    head = max(16, rows // 12 // 16 * 16)
    half = (rows - head) // 2 // 16 * 16
    sizes = [size for size in (head, half, rows - head - half) if size > 0]
    starts = [sum(sizes[:i]) for i in range(len(sizes))]
    return tuple(zip(starts, sizes))


def make_body(mesh):
    n_dp = mesh.shape["dp"]
    experts = mesh.shape["expert"]
    levels = n_dp // CORES

    def body(ag, aw, am, av, eg, ew, hm, hs, count, holder, slot, step):
        depth, cols = ag.shape[1], ag.shape[2]
        rows = depth // n_dp
        cuts = cut_rows(rows)
        maxb, width = eg.shape[2], eg.shape[3]
        slots = hm.shape[1]
        per_holder = max(1, maxb // experts)
        f32 = jnp.float32
        hbm = pl.BlockSpec(memory_space=pltpu.HBM)
        vmem = pl.BlockSpec(memory_space=pltpu.VMEM)
        shape = jax.ShapeDtypeStruct
        moved = (experts, 2, per_holder, width)
        sums, wmv, blocks, scales = pl.pallas_call(
            functools.partial(kernel, levels, experts, per_holder, cuts),
            out_shape=[pltpu.VMEM(s, f32) for s in ((rows, cols), (3, rows, cols), (4, maxb, width), (4, 128))],
            in_specs=[hbm] * 12,
            out_specs=[vmem] * 4,
            scratch_shapes=[
                pltpu.VMEM((levels, CORES, rows, cols), ag.dtype),
                pltpu.VMEM((levels, rows, cols), f32),
                pltpu.VMEM((levels, rows, cols), f32),
                pltpu.VMEM((levels + 1, rows, cols), f32),
                pltpu.VMEM((2, slots, width), f32),
                pltpu.VMEM(moved, f32), pltpu.VMEM(moved, f32),
                pltpu.VMEM((1, 128), f32), pltpu.VMEM((n_dp * experts, 1, 128), f32),
                pltpu.SMEM(count.shape, jnp.int32), pltpu.SMEM(holder.shape, jnp.int32),
                pltpu.SMEM(slot.shape, jnp.int32), pltpu.SMEM(step.shape, jnp.int32),
            ],
            compiler_params=pltpu.CompilerParams(
                collective_id=0, has_side_effects=True, vmem_limit_bytes=LIMIT
            ),
        )(
            *(pltpu.with_memory_space_constraint(x, pltpu.HBM) for x in (
                ag.reshape(levels, CORES, rows, cols), eg[0, 0], ew[0, 0],
                aw, am, av, hm[0], hs[0], count, holder, slot,
            )),
            step,
        )
        outs = pl.pallas_call(
            update,
            out_shape=[shape((rows, cols), f32)] * 3 + [shape((maxb, width), f32)] * 3,
            in_specs=[vmem] * 4,
            out_specs=[hbm] * 6,
            scratch_shapes=[pltpu.VMEM((3, rows, cols), f32), pltpu.VMEM((3, maxb, width), f32), pltpu.SemaphoreType.DMA(()), pltpu.SemaphoreType.DMA(())],
            compiler_params=pltpu.CompilerParams(vmem_limit_bytes=16 * 1024 * 1024),
        )(wmv, sums, blocks, scales)
        return tuple(outs[:3]) + tuple(o[None, None] for o in outs[3:])

    return body


def solution(mesh):
    matrix = P("dp", "expert")
    blocks = P("dp", "expert", None, None)
    held = P("dp", "expert", None)
    return jax.shard_map(
        make_body(mesh),
        mesh=mesh,
        in_specs=(P("dp", None, "expert"), matrix, matrix, matrix, blocks, blocks, held, held, P(), P(), P(), P()),
        out_specs=(matrix, matrix, matrix, blocks, blocks, blocks),
        check_vma=False,
    )
```

```python
import functools

import jax
import jax.numpy as jnp
from jax import lax
from jax.experimental import pallas as pl
from jax.experimental.pallas import tpu as pltpu
from jax.sharding import PartitionSpec as P

MESH = pl.DeviceIdType.MESH
CORES = 2
LIMIT = 40 * 1024 * 1024

beta_first = 0.9
beta_second = 0.95
learn_rate = 0.1
decay_rate = 0.1
adam_epsilon = 1e-08
clip_norm = 1.0


def power(base, exponent):
    result = jnp.float32(1.0)
    value = base
    for bit in range(31):
        factor = value if value > 1e-37 else 0.0
        result = jnp.where((exponent >> bit) & 1 == 1, result * jnp.float32(factor), result)
        value = value * value
    return result


def far_first(size):
    return sorted(range(size), key=lambda k: (-min(k, size - k), k))


def kernel(
    levels, experts, per_holder, cuts,
    grad_hbm, eg_hbm, ew_hbm, w_hbm, m_hbm, v_hbm, hm_hbm, hs_hbm, count_hbm, holder_hbm, slot_hbm, step_hbm,
    sum_ref, wmv, blocks, scale_ref,
    grad, pair_out, local, recv, held, mom_out, mom_in, part, parts, edge_part,
    count_ref, holder_ref, slot_ref, step_ref,
):
    dma = pltpu.SemaphoreType.DMA
    pl.run_scoped(
        functools.partial(
            scoped, levels, experts, per_holder, cuts,
            grad_hbm, eg_hbm, ew_hbm, w_hbm, m_hbm, v_hbm, hm_hbm, hs_hbm, count_hbm, holder_hbm, slot_hbm, step_hbm,
            sum_ref, wmv, blocks, scale_ref,
            grad, pair_out, local, recv, held, mom_out, mom_in, part, parts, edge_part,
            count_ref, holder_ref, slot_ref, step_ref,
        ),
        dma((levels + 1,)), dma((7,)), dma(()), dma((len(cuts) + levels - 1,)),
        dma(()), dma((levels + 1, len(cuts))),
        dma(()), dma(()), dma(()), dma(()), dma(()), dma((2,)),
    )


def scoped(
    levels, experts, per_holder, cuts,
    grad_hbm, eg_hbm, ew_hbm, w_hbm, m_hbm, v_hbm, hm_hbm, hs_hbm, count_hbm, holder_hbm, slot_hbm, step_hbm,
    sum_ref, wmv, blocks, scale_ref,
    grad, pair_out, local, recv, held, mom_out, mom_in, part, parts, edge_part,
    count_ref, holder_ref, slot_ref, step_ref,
    grad_sem, load_sem, pair_send, pair_recv, link_send, link_recv,
    mom_send, mom_recv, part_send, part_recv, back_send, edge_sem,
):
    dp = lax.axis_index("dp")
    me = lax.axis_index("expert")
    z = dp // CORES
    core = dp % CORES
    other = 1 - core
    partner = z * CORES + other
    upper = 2 * z >= levels
    maxb = holder_ref.shape[1]
    rows = sum_ref.shape[0]
    steps = len(cuts)
    devices = levels * CORES * experts
    spans = [pl.ds(start, size) for start, size in cuts]
    kept = sum(start + size <= rows // 2 for start, size in cuts) if levels >= 4 else 0
    near = ((z == 1) | (z == levels - 2)) if kept else False

    def level_of(j):
        return jnp.where(upper, j, levels - 1 - j)

    first = level_of(0)
    head = cuts[0][1]

    def load_level(j):
        d = level_of(j)
        return pltpu.make_async_copy(grad_hbm.at[d], grad.at[d], grad_sem.at[j])

    def load_first(i, start, size):
        span = pl.ds(start, size)
        return pltpu.make_async_copy(grad_hbm.at[first, :, span], grad.at[first, :, span], grad_sem.at[i])

    opening = [load_first(0, 0, head)]
    if rows > head:
        opening.append(load_first(levels, head, rows - head))
    opening[0].start()

    barrier = pltpu.get_barrier_semaphore()
    pl.semaphore_signal(barrier, inc=1, device_id=(partner, me), device_id_type=MESH)

    @pl.when(z > 0)
    def _():
        pl.semaphore_signal(barrier, inc=1, device_id=(dp - CORES, me), device_id_type=MESH)

    @pl.when(z < levels - 1)
    def _():
        pl.semaphore_signal(barrier, inc=1, device_id=(dp + CORES, me), device_id_type=MESH)

    for off in range(1, experts):
        pl.semaphore_signal(barrier, inc=1, device_id=(dp, lax.rem(me + off, experts)), device_id_type=MESH)

    for load in opening[1:]:
        load.start()
    for j in range(1, levels):
        load_level(j).start()

    def pair_copy(d, span, sem):
        return pltpu.make_async_remote_copy(
            src_ref=pair_out.at[d, span], dst_ref=local.at[d, span],
            send_sem=pair_send, recv_sem=pair_recv.at[sem],
            device_id=(partner, me), device_id_type=MESH,
        )

    def link_copy(way, d, p, src, send=link_send):
        slot = d + 1 - way
        return pltpu.make_async_remote_copy(
            src_ref=src, dst_ref=recv.at[slot, spans[p]],
            send_sem=send, recv_sem=link_recv.at[slot, p],
            device_id=(jnp.where(way == 0, dp + CORES, dp - CORES), me), device_id_type=MESH,
        )

    way_out = jnp.where(upper, 1, 0)
    at_end = (z == 0) | (z == levels - 1)

    opening[0].wait()
    pair_out[first, spans[0]] = grad[first, other, spans[0]].astype(jnp.float32)
    linked = jnp.where(z > 0, 1, 0) + jnp.where(z < levels - 1, 1, 0)
    pl.semaphore_wait(barrier, experts + linked)
    pair_copy(first, spans[0], 0).start()
    for load in opening[1:]:
        load.wait()
    for p in range(1, steps):
        pair_out[first, spans[p]] = grad[first, other, spans[p]].astype(jnp.float32)
        pair_copy(first, spans[p], p).start()

    def open_link(p):
        link_copy(way_out, first, p, local.at[first, spans[p]]).start()

    sender = at_end & (first != z)
    late_core = 1
    hold = min(3, steps - 1)
    for p in range(steps):
        pair_copy(first, spans[p], p).wait_recv()
        local[first, spans[p]] = local[first, spans[p]] + grad[first, core, spans[p]].astype(jnp.float32)
        if p == 0 and hold:
            pl.when(sender & (core != late_core))(lambda: open_link(0))
        if p == hold and hold:
            for q in range(hold):
                pl.when(sender & (core == late_core))(lambda: open_link(q))
        if 0 < p < hold:
            pl.when(sender & (core != late_core))(lambda: open_link(p))
        elif p >= hold:
            pl.when(sender)(lambda: open_link(p))

    whole = pl.ds(0, rows)

    def give(j):
        load_level(j).wait()
        d = level_of(j)
        pair_out[d] = grad[d, other].astype(jnp.float32)
        pair_copy(d, whole, steps + j - 1).start()

    def take(j):
        d = level_of(j)
        pair_copy(d, whole, steps + j - 1).wait_recv()
        local[d] = local[d] + grad[d, core].astype(jnp.float32)

        @pl.when(at_end & (j < levels - 2))
        def _():
            for p in range(steps):
                link_copy(way_out, d, p, local.at[d, spans[p]]).start()

        @pl.when(at_end & (j == levels - 2))
        def _():
            for p in reversed(range(kept, steps)):
                link_copy(way_out, d, p, local.at[d, spans[p]]).start()

    ints = [
        pltpu.make_async_copy(a, b, load_sem.at[i])
        for i, (a, b) in enumerate(((count_hbm, count_ref), (holder_hbm, holder_ref), (slot_hbm, slot_ref), (step_hbm, step_ref)))
    ]
    for load in ints:
        load.start()
    for i, source in enumerate((hm_hbm, hs_hbm)):
        pltpu.make_async_copy(source, held.at[i], load_sem.at[4]).start()

    if levels > 1:
        give(1)

    @pl.loop(1, levels)
    def _(j):
        @pl.when(j + 1 < levels)
        def _():
            give(j + 1)

        take(j)

    for i, source in enumerate((w_hbm, m_hbm, v_hbm)):
        pltpu.make_async_copy(source, wmv.at[i], load_sem.at[5]).start()
    for i, source in enumerate((eg_hbm, ew_hbm)):
        pltpu.make_async_copy(source, blocks.at[i], load_sem.at[6]).start()
    for load in ints:
        load.wait()
    pltpu.make_async_copy(held, held, load_sem.at[4]).wait()

    def moment_copy(target, source):
        return pltpu.make_async_remote_copy(
            src_ref=mom_out.at[target], dst_ref=mom_in.at[source],
            send_sem=mom_send, recv_sem=mom_recv,
            device_id=(dp, target), device_id_type=MESH,
        )

    def picks(owner):
        rank = jnp.int32(0)
        chosen = [jnp.int32(0)] * per_holder
        for b in range(maxb):
            mine = (holder_ref[owner, b] == me) & (b < count_ref[owner])
            for q in range(per_holder):
                chosen[q] = jnp.where(mine & (rank == q), slot_ref[owner, b], chosen[q])
            rank = rank + jnp.where(mine, 1, 0)
        return chosen

    for q, slot in enumerate(picks(me)):
        for i in range(2):
            mom_in[me, i, pl.ds(q, 1), :] = held[i, pl.ds(slot, 1), :]

    @pl.loop(1, experts)
    def _(off):
        owner = lax.rem(me + off, experts)
        for q, slot in enumerate(picks(owner)):
            for i in range(2):
                mom_out[owner, i, pl.ds(q, 1), :] = held[i, pl.ds(slot, 1), :]
        moment_copy(owner, me).start()

    def forward(way, j, p):
        d = jnp.where(way == 0, levels - 1 - j, j)
        ahead = jnp.where(way == 0, (d > z) & (z > 0), (d < z) & (z < levels - 1))
        slot = d + 1 - way

        @pl.when(ahead)
        def _():
            block = recv.at[slot, spans[p]]
            copy = link_copy(way, d, p, block)
            copy.wait_recv()
            recv[slot, spans[p]] = recv[slot, spans[p]] + local[d, spans[p]]
            copy.start()

        if p < kept:
            @pl.when((d == z) & (z == jnp.where(way == 0, levels - 2, 1)))
            def _():
                copy = link_copy(way, d, p, recv.at[slot, spans[p]], back_send)
                copy.wait_recv()
                recv[slot, spans[p]] = recv[slot, spans[p]] + local[d, spans[p]]
                copy.start()

    @pl.loop(0, levels)
    def _(j):
        for p in range(steps):
            forward(way_out, j, p)
            if p:
                forward(1 - way_out, j, p - 1)
            else:
                @pl.when(j > 0)
                def _():
                    forward(1 - way_out, j - 1, steps - 1)

    forward(1 - way_out, levels - 1, steps - 1)

    if experts > 1:
        others = mom_in.at[pl.ds(0, experts - 1)]
        pltpu.make_async_copy(others, others, mom_recv).wait()
        others = mom_out.at[pl.ds(0, experts - 1)]
        pltpu.make_async_copy(others, others, mom_send).wait()

    owned = count_ref[me]
    for b in range(maxb):
        holder = holder_ref[me, b]
        rank = jnp.int32(0)
        for earlier in range(b):
            rank = rank + jnp.where((holder_ref[me, earlier] == holder) & (earlier < owned), 1, 0)
        rank = jnp.minimum(rank, per_holder - 1)
        for i in range(2):
            blocks[2 + i, pl.ds(b, 1), :] = mom_in[holder, i, pl.ds(rank, 1), :]
    taken = blocks.at[pl.ds(0, 2)]
    pltpu.make_async_copy(taken, taken, load_sem.at[6]).wait()
    width = blocks.shape[2]
    live = lax.broadcasted_iota(jnp.int32, (maxb, 128), 0) < owned
    acc = jnp.zeros((maxb, 128), jnp.float32)
    for i in range(width // 128):
        span = pl.ds(i * 128, 128)
        g = jnp.where(live, blocks[0, :, span], 0.0)
        w = blocks[1, :, span]
        blocks[0, :, span] = g
        blocks[1, :, span] = jnp.where(live, (1.0 - learn_rate * decay_rate) * w, w)
        blocks[2, :, span] = jnp.where(live, beta_first * blocks[2, :, span], 0.0)
        blocks[3, :, span] = jnp.where(live, beta_second * blocks[3, :, span], 0.0)
        acc = acc + g * g
    row = jnp.sum(acc, axis=0, keepdims=True)
    pltpu.make_async_copy(wmv, wmv, load_sem.at[5]).wait()
    for i, scale in enumerate((1.0 - learn_rate * decay_rate, beta_first, beta_second)):
        wmv[i] = wmv[i] * scale
    step = step_ref[0]
    one = jnp.ones((1, 128), jnp.float32)
    first_left = one * (1.0 - power(beta_first, step))
    second_root = jnp.sqrt(one * (1.0 - power(beta_second, step)))
    scale_ref[2:3] = learn_rate * second_root / first_left
    scale_ref[3:4] = adam_epsilon * second_root

    early = 1 - way_out
    inner = jnp.where(upper, z > 0, z < levels - 1)
    outer = jnp.where(upper, z < levels - 1, z > 0)
    part[...] = row

    def square(ref, at):
        g = ref[at]
        col = jnp.sum(g * g, axis=0, keepdims=True)
        for i in range(g.shape[1] // 128):
            part[...] = part[...] + col[:, i * 128:(i + 1) * 128]

    for p in range(steps):
        taken = near if p < kept else False

        @pl.when(inner & jnp.logical_not(taken))
        def _():
            link_copy(early, z, p, recv.at[z + 1 - early, spans[p]]).wait_recv()
            sum_ref[spans[p]] = local[z, spans[p]] + recv[z + 1 - early, spans[p]]

        @pl.when(jnp.logical_not(inner))
        def _():
            sum_ref[spans[p]] = local[z, spans[p]]

    if kept:
        @pl.when(at_end)
        def _():
            d = level_of(levels - 2)
            slot = d + 1 - early
            for p in range(kept):
                block = recv.at[slot, spans[p]]
                link_copy(early, d, p, block).wait_recv()
                recv[slot, spans[p]] = recv[slot, spans[p]] + local[d, spans[p]]
                square(recv, (slot, spans[p]))

    def last(p):
        link_copy(way_out, z, p, recv.at[z + 1 - way_out, spans[p]]).wait_recv()

    for p in reversed(range(steps)):
        taken = near if p < kept else False

        @pl.when(outer & jnp.logical_not(taken))
        def _():
            last(p)
            sum_ref[spans[p]] = sum_ref[spans[p]] + recv[z + 1 - way_out, spans[p]]

        @pl.when(jnp.logical_not(taken))
        def _():
            square(sum_ref, spans[p])

    inside = devices - 2 * CORES * experts if kept else devices
    index = dp * experts + me - (CORES * experts if kept else 0)

    def part_copy(target_dp, target_me):
        return pltpu.make_async_remote_copy(
            src_ref=part, dst_ref=parts.at[index],
            send_sem=part_send, recv_sem=part_recv,
            device_id=(target_dp, target_me), device_id_type=MESH,
        )

    def spread():
        parts[index] = part[...]
        if devices <= 64:
            for far in far_first(levels):
                side = lax.rem(z + far, levels) * CORES
                for off in far_first(experts):
                    target = lax.rem(me + off, experts)
                    for swap in range(CORES):
                        if far or off or swap:
                            part_copy(side + lax.rem(core + swap, CORES), target).start()
        else:
            @pl.loop(1, devices)
            def _(off):
                target = lax.rem(dp * experts + me + off, devices)
                part_copy(target // experts, lax.rem(target, experts)).start()

    everyone = parts.at[pl.ds(0, devices - 1)]
    if kept:
        edge = pltpu.make_async_remote_copy(
            src_ref=part, dst_ref=edge_part, send_sem=edge_sem.at[0], recv_sem=edge_sem.at[1],
            device_id=(jnp.where(upper, dp - CORES, dp + CORES), me), device_id_type=MESH,
        )

        @pl.when(at_end)
        def _():
            edge.start()
            d = level_of(levels - 2)
            for p in reversed(range(kept)):
                link_copy(way_out, d, p, recv.at[d + 1 - early, spans[p]]).start()

        @pl.when(near)
        def _():
            edge.wait_recv()
            part[...] = part[...] + edge_part[...]

        pl.when(jnp.logical_not(at_end))(spread)
    else:
        spread()

    if kept:
        @pl.when(near)
        def _():
            for p in reversed(range(kept)):
                last(p)
                sum_ref[spans[p]] = recv[z + 1 - way_out, spans[p]]
            back = local.at[0, pl.ds(0, sum(size for _, size in cuts[:kept]))]
            pltpu.make_async_copy(back, back, back_send).wait()

    pltpu.make_async_copy(pair_out, pair_out, pair_send).wait()
    if levels > 1:
        sent = local.at[pl.ds(0, levels - 1)]
        pltpu.make_async_copy(sent, sent, link_send).wait()
    if kept:
        @pl.when(at_end)
        def _():
            edge.wait_send()
            everything = parts.at[pl.ds(0, inside)]
            pltpu.make_async_copy(everything, everything, part_recv).wait()

        @pl.when(jnp.logical_not(at_end))
        def _():
            pltpu.make_async_copy(everyone, everyone, part_send).wait()
            others = parts.at[pl.ds(0, inside - 1)]
            pltpu.make_async_copy(others, others, part_recv).wait()
    else:
        pltpu.make_async_copy(everyone, everyone, part_send).wait()
        pltpu.make_async_copy(everyone, everyone, part_recv).wait()
    total = jnp.sum(jnp.sum(parts[pl.ds(0, inside)], axis=0), axis=1, keepdims=True)
    factor = jnp.broadcast_to(jnp.minimum(1.0, clip_norm / (jnp.sqrt(total) + 1e-06)), (1, 128))
    scale_ref[0:1] = (1.0 - beta_first) * factor
    scale_ref[1:2] = (1.0 - beta_second) ** 0.5 * factor


def update(
    wmv, sums, blocks, scale_ref,
    ow_hbm, om_hbm, ov_hbm, oew_hbm, oem_hbm, oes_hbm,
    out, block_out, sem, block_sem,
):
    first_factor = scale_ref[0:1, 0:1]
    second_factor = scale_ref[1:2, 0:1]
    rate = scale_ref[2:3, 0:1]
    epsilon = scale_ref[3:4, 0:1]
    def chunk(start, size):
        span = pl.ds(start, size)
        g = sums[span]
        m = wmv[1, span] + first_factor * g
        s = second_factor * g
        v = wmv[2, span] + s * s
        out[1, span] = m
        pltpu.make_async_copy(out.at[1, span], om_hbm.at[span], sem).start()
        out[2, span] = v
        pltpu.make_async_copy(out.at[2, span], ov_hbm.at[span], sem).start()
        out[0, span] = wmv[0, span] - rate * m / (v * lax.rsqrt(v) + epsilon)
        pltpu.make_async_copy(out.at[0, span], ow_hbm.at[span], sem).start()

    rows = sums.shape[0]
    for start, size in chunk_rows(rows):
        chunk(start, size)

    width = blocks.shape[2]
    for i in range(width // 128):
        cols = pl.ds(i * 128, 128)
        g = blocks[0, :, cols]
        m = blocks[2, :, cols] + first_factor * g
        s = second_factor * g
        v = blocks[3, :, cols] + s * s
        block_out[1, :, cols] = m
        block_out[2, :, cols] = v
        block_out[0, :, cols] = blocks[1, :, cols] - rate * m / (jnp.sqrt(v) + epsilon)
    for i, dst in enumerate((oew_hbm, oem_hbm, oes_hbm)):
        pltpu.make_async_copy(block_out.at[i], dst, block_sem).start()
    pltpu.make_async_copy(out, out, sem).wait()
    pltpu.make_async_copy(block_out, block_out, block_sem).wait()


def chunk_rows(rows):
    unit = rows // 8 // 8 * 8
    if not unit or rows % 8:
        return ((0, rows),)
    sizes = [unit, 2 * unit, 2 * unit, rows - 5 * unit]
    return tuple((sum(sizes[:i]), sizes[i]) for i in range(4))


def cut_rows(rows):
    unit = rows // 6 // 16 * 16
    if not unit or rows % 16:
        return ((0, rows),)
    half = unit // 2 // 16 * 16
    sizes = ([half, unit - half] if half else [unit]) + [unit] * ((rows - unit) // unit)
    if rows > sum(sizes):
        sizes.append(rows - sum(sizes))
    return tuple((sum(sizes[:i]), sizes[i]) for i in range(len(sizes)))


def make_body(mesh):
    n_dp = mesh.shape["dp"]
    experts = mesh.shape["expert"]
    levels = n_dp // CORES

    def body(ag, aw, am, av, eg, ew, hm, hs, count, holder, slot, step):
        depth, cols = ag.shape[1], ag.shape[2]
        rows = depth // n_dp
        cuts = cut_rows(rows)
        maxb, width = eg.shape[2], eg.shape[3]
        slots = hm.shape[1]
        per_holder = max(1, maxb // experts)
        f32 = jnp.float32
        hbm = pl.BlockSpec(memory_space=pltpu.HBM)
        vmem = pl.BlockSpec(memory_space=pltpu.VMEM)
        shape = jax.ShapeDtypeStruct
        moved = (experts, 2, per_holder, width)
        sums, wmv, blocks, scales = pl.pallas_call(
            functools.partial(kernel, levels, experts, per_holder, cuts),
            out_shape=[pltpu.VMEM(s, f32) for s in ((rows, cols), (3, rows, cols), (4, maxb, width), (4, 128))],
            in_specs=[hbm] * 12,
            out_specs=[vmem] * 4,
            scratch_shapes=[
                pltpu.VMEM((levels, CORES, rows, cols), ag.dtype),
                pltpu.VMEM((levels, rows, cols), f32),
                pltpu.VMEM((levels, rows, cols), f32),
                pltpu.VMEM((levels + 1, rows, cols), f32),
                pltpu.VMEM((2, slots, width), f32),
                pltpu.VMEM(moved, f32), pltpu.VMEM(moved, f32),
                pltpu.VMEM((1, 128), f32), pltpu.VMEM((n_dp * experts, 1, 128), f32), pltpu.VMEM((1, 128), f32),
                pltpu.SMEM(count.shape, jnp.int32), pltpu.SMEM(holder.shape, jnp.int32),
                pltpu.SMEM(slot.shape, jnp.int32), pltpu.SMEM(step.shape, jnp.int32),
            ],
            compiler_params=pltpu.CompilerParams(
                collective_id=0, has_side_effects=True, vmem_limit_bytes=LIMIT
            ),
        )(
            *(pltpu.with_memory_space_constraint(x, pltpu.HBM) for x in (
                ag.reshape(levels, CORES, rows, cols), eg[0, 0], ew[0, 0],
                aw, am, av, hm[0], hs[0], count, holder, slot,
            )),
            step,
        )
        outs = pl.pallas_call(
            update,
            out_shape=[shape((rows, cols), f32)] * 3 + [shape((maxb, width), f32)] * 3,
            in_specs=[vmem] * 4,
            out_specs=[hbm] * 6,
            scratch_shapes=[pltpu.VMEM((3, rows, cols), f32), pltpu.VMEM((3, maxb, width), f32), pltpu.SemaphoreType.DMA(()), pltpu.SemaphoreType.DMA(())],
            compiler_params=pltpu.CompilerParams(vmem_limit_bytes=16 * 1024 * 1024),
        )(wmv, sums, blocks, scales)
        return tuple(outs[:3]) + tuple(o[None, None] for o in outs[3:])

    return body


def solution(mesh):
    matrix = P("dp", "expert")
    blocks = P("dp", "expert", None, None)
    held = P("dp", "expert", None)
    return jax.shard_map(
        make_body(mesh),
        mesh=mesh,
        in_specs=(P("dp", None, "expert"), matrix, matrix, matrix, blocks, blocks, held, held, P(), P(), P(), P()),
        out_specs=(matrix, matrix, matrix, blocks, blocks, blocks),
        check_vma=False,
    )
```

```python
import functools

import jax
import jax.numpy as jnp
from jax import lax
from jax.experimental import pallas as pl
from jax.experimental.pallas import tpu as pltpu
from jax.sharding import PartitionSpec as P

MESH = pl.DeviceIdType.MESH
CORES = 2
WRITES = 4
LIMIT = 40 * 1024 * 1024

beta_first = 0.9
beta_second = 0.95
learn_rate = 0.1
decay_rate = 0.1
adam_epsilon = 1e-08
clip_norm = 1.0


def power(base, exponent):
    result = jnp.float32(1.0)
    value = base
    for bit in range(31):
        factor = value if value > 1e-37 else 0.0
        result = jnp.where((exponent >> bit) & 1 == 1, result * jnp.float32(factor), result)
        value = value * value
    return result


def far_first(size):
    return sorted(range(size), key=lambda k: (-min(k, size - k), k))


def kernel(
    levels, experts, per_holder, cuts,
    grad_hbm, eg_hbm, ew_hbm, w_hbm, m_hbm, v_hbm, hm_hbm, hs_hbm, count_hbm, holder_hbm, slot_hbm, step_hbm,
    wmv, blocks,
    sum_ref, scale_ref, grad, pair_out, local, recv, held, mom_out, mom_in, part, parts, edge_part,
    count_ref, holder_ref, slot_ref, step_ref,
):
    dma = pltpu.SemaphoreType.DMA
    pl.run_scoped(
        functools.partial(
            scoped, levels, experts, per_holder, cuts,
            grad_hbm, eg_hbm, ew_hbm, w_hbm, m_hbm, v_hbm, hm_hbm, hs_hbm, count_hbm, holder_hbm, slot_hbm, step_hbm,
            wmv, blocks,
            sum_ref, scale_ref, grad, pair_out, local, recv, held, mom_out, mom_in, part, parts, edge_part,
            count_ref, holder_ref, slot_ref, step_ref,
        ),
        dma((levels + 1,)), dma((7,)), dma(()), dma((len(cuts) + levels - 1,)),
        dma(()), dma((levels + 1, len(cuts))),
        dma(()), dma(()), dma(()), dma(()), dma(()), dma((2,)),
        pltpu.SemaphoreType.REGULAR, pltpu.SemaphoreType.REGULAR,
    )


def scoped(
    levels, experts, per_holder, cuts,
    grad_hbm, eg_hbm, ew_hbm, w_hbm, m_hbm, v_hbm, hm_hbm, hs_hbm, count_hbm, holder_hbm, slot_hbm, step_hbm,
    wmv, blocks,
    sum_ref, scale_ref, grad, pair_out, local, recv, held, mom_out, mom_in, part, parts, edge_part,
    count_ref, holder_ref, slot_ref, step_ref,
    grad_sem, load_sem, pair_send, pair_recv, link_send, link_recv,
    mom_send, mom_recv, part_send, part_recv, back_send, edge_sem, ready_sem, open_sem,
):
    dp = lax.axis_index("dp")
    me = lax.axis_index("expert")
    z = dp // CORES
    core = dp % CORES
    other = 1 - core
    partner = z * CORES + other
    upper = 2 * z >= levels
    maxb = holder_ref.shape[1]
    rows = sum_ref.shape[0]
    steps = len(cuts)
    devices = levels * CORES * experts
    spans = [pl.ds(start, size) for start, size in cuts]
    kept = sum(start + size <= rows // 2 for start, size in cuts) if levels >= 4 else 0
    near = ((z == 1) | (z == levels - 2)) if kept else False

    def level_of(j):
        return jnp.where(upper, j, levels - 1 - j)

    first = level_of(0)
    head = cuts[0][1]

    def load_level(j):
        d = level_of(j)
        return pltpu.make_async_copy(grad_hbm.at[d], grad.at[d], grad_sem.at[j])

    def load_first(i, start, size):
        span = pl.ds(start, size)
        return pltpu.make_async_copy(grad_hbm.at[first, :, span], grad.at[first, :, span], grad_sem.at[i])

    opening = [load_first(0, 0, head)]
    if rows > head:
        opening.append(load_first(levels, head, rows - head))
    opening[0].start()

    at_end = (z == 0) | (z == levels - 1)
    barrier = pltpu.get_barrier_semaphore()
    pl.semaphore_signal(barrier, inc=1, device_id=(partner, me), device_id_type=MESH)

    @pl.when(z > 0)
    def _():
        pl.semaphore_signal(barrier, inc=1, device_id=(dp - CORES, me), device_id_type=MESH)

    @pl.when(z < levels - 1)
    def _():
        pl.semaphore_signal(barrier, inc=1, device_id=(dp + CORES, me), device_id_type=MESH)

    def greet(sem):
        for off in range(1, experts):
            pl.semaphore_signal(sem, inc=1, device_id=(dp, lax.rem(me + off, experts)), device_id_type=MESH)

    if kept:
        pl.when(jnp.logical_not(at_end))(lambda: greet(barrier))
    else:
        greet(barrier)

    for load in opening[1:]:
        load.start()
    for j in range(1, levels):
        load_level(j).start()

    def pair_copy(d, span, sem):
        return pltpu.make_async_remote_copy(
            src_ref=pair_out.at[d, span], dst_ref=local.at[d, span],
            send_sem=pair_send, recv_sem=pair_recv.at[sem],
            device_id=(partner, me), device_id_type=MESH,
        )

    def link_copy(way, d, p, src, send=link_send):
        slot = d + 1 - way
        return pltpu.make_async_remote_copy(
            src_ref=src, dst_ref=recv.at[slot, spans[p]],
            send_sem=send, recv_sem=link_recv.at[slot, p],
            device_id=(jnp.where(way == 0, dp + CORES, dp - CORES), me), device_id_type=MESH,
        )

    way_out = jnp.where(upper, 1, 0)

    opening[0].wait()
    pair_out[first, spans[0]] = grad[first, other, spans[0]].astype(jnp.float32)
    linked = jnp.where(z > 0, 1, 0) + jnp.where(z < levels - 1, 1, 0)
    crossed = jnp.where(at_end, 0, experts - 1) if kept else experts - 1
    pl.semaphore_wait(barrier, 1 + linked + crossed)
    pair_copy(first, spans[0], 0).start()
    for load in opening[1:]:
        load.wait()
    for p in range(1, steps):
        pair_out[first, spans[p]] = grad[first, other, spans[p]].astype(jnp.float32)
        pair_copy(first, spans[p], p).start()

    def open_link(p):
        link_copy(way_out, first, p, local.at[first, spans[p]]).start()

    sender = at_end & (first != z)
    late_core = 1
    hold = min(3, steps - 1)
    for p in range(steps):
        pair_copy(first, spans[p], p).wait_recv()
        local[first, spans[p]] = local[first, spans[p]] + grad[first, core, spans[p]].astype(jnp.float32)
        if p == 0 and hold:
            pl.when(sender & (core != late_core))(lambda: open_link(0))
        if p == hold and hold:
            for q in range(hold):
                pl.when(sender & (core == late_core))(lambda: open_link(q))
        if 0 < p < hold:
            pl.when(sender & (core != late_core))(lambda: open_link(p))
        elif p >= hold:
            pl.when(sender)(lambda: open_link(p))

    whole = pl.ds(0, rows)

    def give(j):
        load_level(j).wait()
        d = level_of(j)
        pair_out[d] = grad[d, other].astype(jnp.float32)
        pair_copy(d, whole, steps + j - 1).start()

    def take(j):
        d = level_of(j)
        pair_copy(d, whole, steps + j - 1).wait_recv()
        local[d] = local[d] + grad[d, core].astype(jnp.float32)

        @pl.when(at_end & (j < levels - 2))
        def _():
            for p in range(steps):
                link_copy(way_out, d, p, local.at[d, spans[p]]).start()

        @pl.when(at_end & (j == levels - 2))
        def _():
            for p in reversed(range(kept, steps)):
                link_copy(way_out, d, p, local.at[d, spans[p]]).start()

    ints = [
        pltpu.make_async_copy(a, b, load_sem.at[i])
        for i, (a, b) in enumerate(((count_hbm, count_ref), (holder_hbm, holder_ref), (slot_hbm, slot_ref), (step_hbm, step_ref)))
    ]
    for load in ints:
        load.start()
    for i, source in enumerate((hm_hbm, hs_hbm)):
        pltpu.make_async_copy(source, held.at[i], load_sem.at[4]).start()

    if levels > 1:
        give(1)

    @pl.loop(1, levels)
    def _(j):
        @pl.when(j + 1 < levels)
        def _():
            give(j + 1)

        take(j)

    if kept:
        pl.when(near)(lambda: greet(ready_sem))
    for i, source in enumerate((w_hbm, m_hbm, v_hbm)):
        pltpu.make_async_copy(source, wmv.at[i], load_sem.at[5]).start()
    for i, source in enumerate((eg_hbm, ew_hbm)):
        pltpu.make_async_copy(source, blocks.at[i], load_sem.at[6]).start()
    for load in ints:
        load.wait()
    pltpu.make_async_copy(held, held, load_sem.at[4]).wait()

    def moment_copy(target, source):
        return pltpu.make_async_remote_copy(
            src_ref=mom_out.at[target], dst_ref=mom_in.at[source],
            send_sem=mom_send, recv_sem=mom_recv,
            device_id=(dp, target), device_id_type=MESH,
        )

    def picks(owner):
        rank = jnp.int32(0)
        chosen = [jnp.int32(0)] * per_holder
        for b in range(maxb):
            mine = (holder_ref[owner, b] == me) & (b < count_ref[owner])
            for q in range(per_holder):
                chosen[q] = jnp.where(mine & (rank == q), slot_ref[owner, b], chosen[q])
            rank = rank + jnp.where(mine, 1, 0)
        return chosen

    if kept:
        @pl.when(near)
        def _():
            pl.semaphore_wait(ready_sem, experts - 1)
            edge_dp = jnp.where(upper, dp + CORES, dp - CORES)
            pl.semaphore_signal(open_sem, inc=1, device_id=(edge_dp, me), device_id_type=MESH)

        @pl.when(at_end)
        def _():
            pl.semaphore_wait(open_sem, 1)

    for q, slot in enumerate(picks(me)):
        for i in range(2):
            mom_in[me, i, pl.ds(q, 1), :] = held[i, pl.ds(slot, 1), :]

    @pl.loop(1, experts)
    def _(off):
        owner = lax.rem(me + off, experts)
        for q, slot in enumerate(picks(owner)):
            for i in range(2):
                mom_out[owner, i, pl.ds(q, 1), :] = held[i, pl.ds(slot, 1), :]
        moment_copy(owner, me).start()

    def forward(way, j, p):
        d = jnp.where(way == 0, levels - 1 - j, j)
        ahead = jnp.where(way == 0, (d > z) & (z > 0), (d < z) & (z < levels - 1))
        slot = d + 1 - way

        @pl.when(ahead)
        def _():
            block = recv.at[slot, spans[p]]
            copy = link_copy(way, d, p, block)
            copy.wait_recv()
            recv[slot, spans[p]] = recv[slot, spans[p]] + local[d, spans[p]]
            copy.start()

        if p < kept:
            @pl.when((d == z) & (z == jnp.where(way == 0, levels - 2, 1)))
            def _():
                copy = link_copy(way, d, p, recv.at[slot, spans[p]], back_send)
                copy.wait_recv()
                recv[slot, spans[p]] = recv[slot, spans[p]] + local[d, spans[p]]
                copy.start()

    @pl.loop(0, levels)
    def _(j):
        for p in range(steps):
            forward(way_out, j, p)
            if p:
                forward(1 - way_out, j, p - 1)
            else:
                @pl.when(j > 0)
                def _():
                    forward(1 - way_out, j - 1, steps - 1)

    forward(1 - way_out, levels - 1, steps - 1)

    if experts > 1:
        others = mom_in.at[pl.ds(0, experts - 1)]
        pltpu.make_async_copy(others, others, mom_recv).wait()
        others = mom_out.at[pl.ds(0, experts - 1)]
        pltpu.make_async_copy(others, others, mom_send).wait()

    owned = count_ref[me]
    for b in range(maxb):
        holder = holder_ref[me, b]
        rank = jnp.int32(0)
        for earlier in range(b):
            rank = rank + jnp.where((holder_ref[me, earlier] == holder) & (earlier < owned), 1, 0)
        rank = jnp.minimum(rank, per_holder - 1)
        for i in range(2):
            blocks[2 + i, pl.ds(b, 1), :] = mom_in[holder, i, pl.ds(rank, 1), :]
    taken = blocks.at[pl.ds(0, 2)]
    pltpu.make_async_copy(taken, taken, load_sem.at[6]).wait()
    width = blocks.shape[2]
    live = lax.broadcasted_iota(jnp.int32, (maxb, 128), 0) < owned
    acc = jnp.zeros((maxb, 128), jnp.float32)
    for i in range(width // 128):
        span = pl.ds(i * 128, 128)
        g = jnp.where(live, blocks[0, :, span], 0.0)
        w = blocks[1, :, span]
        blocks[0, :, span] = g
        blocks[1, :, span] = jnp.where(live, (1.0 - learn_rate * decay_rate) * w, w)
        blocks[2, :, span] = jnp.where(live, beta_first * blocks[2, :, span], 0.0)
        blocks[3, :, span] = jnp.where(live, beta_second * blocks[3, :, span], 0.0)
        acc = acc + g * g
    row = jnp.sum(acc, axis=0, keepdims=True)
    pltpu.make_async_copy(wmv, wmv, load_sem.at[5]).wait()
    for i, scale in enumerate((1.0 - learn_rate * decay_rate, beta_first, beta_second)):
        wmv[i] = wmv[i] * scale
    step = step_ref[0]
    one = jnp.ones((1, 128), jnp.float32)
    first_left = one * (1.0 - power(beta_first, step))
    second_root = jnp.sqrt(one * (1.0 - power(beta_second, step)))
    scale_ref[2:3] = learn_rate * second_root / first_left
    scale_ref[3:4] = adam_epsilon * second_root

    early = 1 - way_out
    inner = jnp.where(upper, z > 0, z < levels - 1)
    outer = jnp.where(upper, z < levels - 1, z > 0)
    part[...] = row

    def square(ref, at):
        g = ref[at]
        col = jnp.sum(g * g, axis=0, keepdims=True)
        for i in range(g.shape[1] // 128):
            part[...] = part[...] + col[:, i * 128:(i + 1) * 128]

    for p in range(steps):
        taken = near if p < kept else False

        @pl.when(inner & jnp.logical_not(taken))
        def _():
            link_copy(early, z, p, recv.at[z + 1 - early, spans[p]]).wait_recv()
            sum_ref[spans[p]] = local[z, spans[p]] + recv[z + 1 - early, spans[p]]

        @pl.when(jnp.logical_not(inner))
        def _():
            sum_ref[spans[p]] = local[z, spans[p]]

    if kept:
        @pl.when(at_end)
        def _():
            d = level_of(levels - 2)
            slot = d + 1 - early
            for p in range(kept):
                block = recv.at[slot, spans[p]]
                link_copy(early, d, p, block).wait_recv()
                recv[slot, spans[p]] = recv[slot, spans[p]] + local[d, spans[p]]
                square(recv, (slot, spans[p]))

    def last(p):
        link_copy(way_out, z, p, recv.at[z + 1 - way_out, spans[p]]).wait_recv()

    for p in reversed(range(steps)):
        taken = near if p < kept else False

        @pl.when(outer & jnp.logical_not(taken))
        def _():
            last(p)
            sum_ref[spans[p]] = sum_ref[spans[p]] + recv[z + 1 - way_out, spans[p]]

        @pl.when(jnp.logical_not(taken))
        def _():
            square(sum_ref, spans[p])

    inside = devices - 2 * CORES * experts if kept else devices
    index = dp * experts + me - (CORES * experts if kept else 0)

    def part_copy(target_dp, target_me):
        return pltpu.make_async_remote_copy(
            src_ref=part, dst_ref=parts.at[index],
            send_sem=part_send, recv_sem=part_recv,
            device_id=(target_dp, target_me), device_id_type=MESH,
        )

    def spread():
        parts[index] = part[...]
        if devices <= 64:
            for far in far_first(levels):
                side = lax.rem(z + far, levels) * CORES
                for off in far_first(experts):
                    target = lax.rem(me + off, experts)
                    for swap in range(CORES):
                        if far or off or swap:
                            part_copy(side + lax.rem(core + swap, CORES), target).start()
        else:
            @pl.loop(1, devices)
            def _(off):
                target = lax.rem(dp * experts + me + off, devices)
                part_copy(target // experts, lax.rem(target, experts)).start()

    if kept:
        edge = pltpu.make_async_remote_copy(
            src_ref=part, dst_ref=edge_part, send_sem=edge_sem.at[0], recv_sem=edge_sem.at[1],
            device_id=(jnp.where(upper, dp - CORES, dp + CORES), me), device_id_type=MESH,
        )

        @pl.when(at_end)
        def _():
            edge.start()
            d = level_of(levels - 2)
            for p in reversed(range(kept)):
                link_copy(way_out, d, p, recv.at[d + 1 - early, spans[p]]).start()

        @pl.when(near)
        def _():
            edge.wait_recv()
            part[...] = part[...] + edge_part[...]

        pl.when(jnp.logical_not(at_end))(spread)
    else:
        spread()

    everyone = parts.at[pl.ds(0, devices - 1)]
    if kept:
        @pl.when(at_end)
        def _():
            everything = parts.at[pl.ds(0, inside)]
            pltpu.make_async_copy(everything, everything, part_recv).wait()

        @pl.when(jnp.logical_not(at_end))
        def _():
            others = parts.at[pl.ds(0, inside - 1)]
            pltpu.make_async_copy(others, others, part_recv).wait()
    else:
        pltpu.make_async_copy(everyone, everyone, part_recv).wait()
    total = jnp.sum(jnp.sum(parts[pl.ds(0, inside)], axis=0), axis=1, keepdims=True)
    factor = jnp.broadcast_to(jnp.minimum(1.0, clip_norm / (jnp.sqrt(total) + 1e-06)), (1, 128))
    scale_ref[0:1] = (1.0 - beta_first) * factor
    scale_ref[1:2] = (1.0 - beta_second) ** 0.5 * factor

    def finish(span, g):
        m = wmv[1, span] + scale_ref[0:1, 0:1] * g
        s = scale_ref[1:2, 0:1] * g
        v = wmv[2, span] + s * s
        wmv[1, span] = m
        wmv[2, span] = v
        wmv[0, span] = wmv[0, span] - scale_ref[2:3, 0:1] * m / (v * lax.rsqrt(v) + scale_ref[3:4, 0:1])

    for p in range(kept, steps):
        finish(spans[p], sum_ref[spans[p]])
    for i in range(width // 128):
        span = pl.ds(i * 128, 128)
        g = blocks[0, :, span]
        m = blocks[2, :, span] + scale_ref[0:1, 0:1] * g
        s = scale_ref[1:2, 0:1] * g
        v = blocks[3, :, span] + s * s
        blocks[2, :, span] = m
        blocks[3, :, span] = v
        blocks[1, :, span] = blocks[1, :, span] - scale_ref[2:3, 0:1] * m / (jnp.sqrt(v) + scale_ref[3:4, 0:1])
    if kept:
        @pl.when(jnp.logical_not(near))
        def _():
            for p in range(kept):
                finish(spans[p], sum_ref[spans[p]])

    pltpu.make_async_copy(pair_out, pair_out, pair_send).wait()
    if levels > 1:
        sent = local.at[pl.ds(0, levels - 1)]
        pltpu.make_async_copy(sent, sent, link_send).wait()
    if kept:
        @pl.when(at_end)
        def _():
            edge.wait_send()

        @pl.when(jnp.logical_not(at_end))
        def _():
            pltpu.make_async_copy(everyone, everyone, part_send).wait()

        @pl.when(near)
        def _():
            back = local.at[0, pl.ds(0, sum(size for _, size in cuts[:kept]))]
            pltpu.make_async_copy(back, back, back_send).wait()
            for p in reversed(range(kept)):
                last(p)
                finish(spans[p], recv[z + 1 - way_out, spans[p]])
    else:
        pltpu.make_async_copy(everyone, everyone, part_send).wait()


def write(parts, wmv, blocks, ow_hbm, om_hbm, ov_hbm, oew_hbm, oem_hbm, oes_hbm, sem, block_sem):
    size = wmv.shape[1] // parts
    for k in range(parts):
        span = pl.ds(k * size, size)
        for i, dst in enumerate((ow_hbm, om_hbm, ov_hbm)):
            pltpu.make_async_copy(wmv.at[i, span], dst.at[span], sem).start()
    for i, dst in enumerate((oew_hbm, oem_hbm, oes_hbm)):
        pltpu.make_async_copy(blocks.at[i + 1], dst, block_sem).start()
    done = blocks.at[pl.ds(1, 3)]
    pltpu.make_async_copy(wmv, wmv, sem).wait()
    pltpu.make_async_copy(done, done, block_sem).wait()


def cut_rows(rows):
    unit = rows // 6 // 16 * 16
    if not unit or rows % 16:
        return ((0, rows),)
    half = unit // 2 // 16 * 16
    sizes = ([half, unit - half] if half else [unit]) + [unit] * ((rows - unit) // unit)
    if rows > sum(sizes):
        sizes.append(rows - sum(sizes))
    return tuple((sum(sizes[:i]), sizes[i]) for i in range(len(sizes)))


def make_body(mesh):
    n_dp = mesh.shape["dp"]
    experts = mesh.shape["expert"]
    levels = n_dp // CORES

    def body(ag, aw, am, av, eg, ew, hm, hs, count, holder, slot, step):
        depth, cols = ag.shape[1], ag.shape[2]
        rows = depth // n_dp
        cuts = cut_rows(rows)
        maxb, width = eg.shape[2], eg.shape[3]
        slots = hm.shape[1]
        per_holder = max(1, maxb // experts)
        f32 = jnp.float32
        hbm = pl.BlockSpec(memory_space=pltpu.HBM)
        vmem = pl.BlockSpec(memory_space=pltpu.VMEM)
        shape = jax.ShapeDtypeStruct
        moved = (experts, 2, per_holder, width)
        wmv, blocks = pl.pallas_call(
            functools.partial(kernel, levels, experts, per_holder, cuts),
            out_shape=[pltpu.VMEM(s, f32) for s in ((3, rows, cols), (4, maxb, width))],
            in_specs=[hbm] * 12,
            out_specs=[vmem] * 2,
            scratch_shapes=[
                pltpu.VMEM((rows, cols), f32), pltpu.VMEM((4, 128), f32),
                pltpu.VMEM((levels, CORES, rows, cols), ag.dtype),
                pltpu.VMEM((levels, rows, cols), f32),
                pltpu.VMEM((levels, rows, cols), f32),
                pltpu.VMEM((levels + 1, rows, cols), f32),
                pltpu.VMEM((2, slots, width), f32),
                pltpu.VMEM(moved, f32), pltpu.VMEM(moved, f32),
                pltpu.VMEM((1, 128), f32), pltpu.VMEM((n_dp * experts, 1, 128), f32), pltpu.VMEM((1, 128), f32),
                pltpu.SMEM(count.shape, jnp.int32), pltpu.SMEM(holder.shape, jnp.int32),
                pltpu.SMEM(slot.shape, jnp.int32), pltpu.SMEM(step.shape, jnp.int32),
            ],
            compiler_params=pltpu.CompilerParams(
                collective_id=0, has_side_effects=True, vmem_limit_bytes=LIMIT
            ),
        )(
            *(pltpu.with_memory_space_constraint(x, pltpu.HBM) for x in (
                ag.reshape(levels, CORES, rows, cols), eg[0, 0], ew[0, 0],
                aw, am, av, hm[0], hs[0], count, holder, slot,
            )),
            step,
        )
        outs = pl.pallas_call(
            functools.partial(write, WRITES if rows % (8 * WRITES) == 0 else 1),
            out_shape=[shape((rows, cols), f32)] * 3 + [shape((maxb, width), f32)] * 3,
            in_specs=[vmem] * 2,
            out_specs=[hbm] * 6,
            scratch_shapes=[pltpu.SemaphoreType.DMA(()), pltpu.SemaphoreType.DMA(())],
            compiler_params=pltpu.CompilerParams(vmem_limit_bytes=16 * 1024 * 1024),
        )(wmv, blocks)
        return tuple(outs[:3]) + tuple(o[None, None] for o in outs[3:])

    return body


def solution(mesh):
    matrix = P("dp", "expert")
    blocks = P("dp", "expert", None, None)
    held = P("dp", "expert", None)
    return jax.shard_map(
        make_body(mesh),
        mesh=mesh,
        in_specs=(P("dp", None, "expert"), matrix, matrix, matrix, blocks, blocks, held, held, P(), P(), P(), P()),
        out_specs=(matrix, matrix, matrix, blocks, blocks, blocks),
        check_vma=False,
    )
```

```python
import functools

import jax
import jax.numpy as jnp
from jax import lax
from jax.experimental import pallas as pl
from jax.experimental.pallas import tpu as pltpu
from jax.sharding import PartitionSpec as P

MESH = pl.DeviceIdType.MESH
CORES = 2
WRITES = 4
LAG = 2
LIMIT = 40 * 1024 * 1024

beta_first = 0.9
beta_second = 0.95
learn_rate = 0.1
decay_rate = 0.1
adam_epsilon = 1e-08
clip_norm = 1.0


def power(base, exponent):
    result = jnp.float32(1.0)
    value = base
    for bit in range(31):
        factor = value if value > 1e-37 else 0.0
        result = jnp.where((exponent >> bit) & 1 == 1, result * jnp.float32(factor), result)
        value = value * value
    return result


def far_first(size):
    return sorted(range(size), key=lambda k: (-min(k, size - k), k))


def kernel(
    levels, experts, per_holder, cuts,
    grad_hbm, eg_hbm, ew_hbm, w_hbm, m_hbm, v_hbm, hm_hbm, hs_hbm, count_hbm, holder_hbm, slot_hbm, step_hbm,
    wmv, blocks,
    sum_ref, scale_ref, grad, pair_out, local, recv, held, mom_out, mom_in, part, parts, edge_part,
    count_ref, holder_ref, slot_ref, step_ref,
):
    dma = pltpu.SemaphoreType.DMA
    pl.run_scoped(
        functools.partial(
            scoped, levels, experts, per_holder, cuts,
            grad_hbm, eg_hbm, ew_hbm, w_hbm, m_hbm, v_hbm, hm_hbm, hs_hbm, count_hbm, holder_hbm, slot_hbm, step_hbm,
            wmv, blocks,
            sum_ref, scale_ref, grad, pair_out, local, recv, held, mom_out, mom_in, part, parts, edge_part,
            count_ref, holder_ref, slot_ref, step_ref,
        ),
        dma((levels + 1,)), dma((7,)), dma(()), dma((len(cuts) + levels - 1,)),
        dma(()), dma((levels + 1, len(cuts))),
        dma(()), dma(()), dma(()), dma(()), dma(()), dma((2,)),
        pltpu.SemaphoreType.REGULAR, pltpu.SemaphoreType.REGULAR,
    )


def scoped(
    levels, experts, per_holder, cuts,
    grad_hbm, eg_hbm, ew_hbm, w_hbm, m_hbm, v_hbm, hm_hbm, hs_hbm, count_hbm, holder_hbm, slot_hbm, step_hbm,
    wmv, blocks,
    sum_ref, scale_ref, grad, pair_out, local, recv, held, mom_out, mom_in, part, parts, edge_part,
    count_ref, holder_ref, slot_ref, step_ref,
    grad_sem, load_sem, pair_send, pair_recv, link_send, link_recv,
    mom_send, mom_recv, part_send, part_recv, back_send, edge_sem, ready_sem, open_sem,
):
    dp = lax.axis_index("dp")
    me = lax.axis_index("expert")
    z = dp // CORES
    core = dp % CORES
    other = 1 - core
    partner = z * CORES + other
    upper = 2 * z >= levels
    maxb = holder_ref.shape[1]
    rows = sum_ref.shape[0]
    steps = len(cuts)
    devices = levels * CORES * experts
    spans = [pl.ds(start, size) for start, size in cuts]
    kept = sum(start + size <= rows // 2 for start, size in cuts) if levels >= 4 else 0
    near = ((z == 1) | (z == levels - 2)) if kept else False

    def level_of(j):
        return jnp.where(upper, j, levels - 1 - j)

    first = level_of(0)
    head = cuts[0][1]

    def load_level(j):
        d = level_of(j)
        return pltpu.make_async_copy(grad_hbm.at[d], grad.at[d], grad_sem.at[j])

    def load_first(i, start, size):
        span = pl.ds(start, size)
        return pltpu.make_async_copy(grad_hbm.at[first, :, span], grad.at[first, :, span], grad_sem.at[i])

    opening = [load_first(0, 0, head)]
    if rows > head:
        opening.append(load_first(levels, head, rows - head))
    opening[0].start()

    at_end = (z == 0) | (z == levels - 1)
    barrier = pltpu.get_barrier_semaphore()
    pl.semaphore_signal(barrier, inc=1, device_id=(partner, me), device_id_type=MESH)

    @pl.when(z > 0)
    def _():
        pl.semaphore_signal(barrier, inc=1, device_id=(dp - CORES, me), device_id_type=MESH)

    @pl.when(z < levels - 1)
    def _():
        pl.semaphore_signal(barrier, inc=1, device_id=(dp + CORES, me), device_id_type=MESH)

    def greet(sem):
        for off in range(1, experts):
            pl.semaphore_signal(sem, inc=1, device_id=(dp, lax.rem(me + off, experts)), device_id_type=MESH)

    if kept:
        pl.when(jnp.logical_not(at_end))(lambda: greet(barrier))
    else:
        greet(barrier)

    for load in opening[1:]:
        load.start()
    for j in range(1, levels):
        load_level(j).start()

    def pair_copy(d, span, sem):
        return pltpu.make_async_remote_copy(
            src_ref=pair_out.at[d, span], dst_ref=local.at[d, span],
            send_sem=pair_send, recv_sem=pair_recv.at[sem],
            device_id=(partner, me), device_id_type=MESH,
        )

    def link_copy(way, d, p, src, send=link_send):
        slot = d + 1 - way
        return pltpu.make_async_remote_copy(
            src_ref=src, dst_ref=recv.at[slot, spans[p]],
            send_sem=send, recv_sem=link_recv.at[slot, p],
            device_id=(jnp.where(way == 0, dp + CORES, dp - CORES), me), device_id_type=MESH,
        )

    way_out = jnp.where(upper, 1, 0)

    opening[0].wait()
    pair_out[first, spans[0]] = grad[first, other, spans[0]].astype(jnp.float32)
    linked = jnp.where(z > 0, 1, 0) + jnp.where(z < levels - 1, 1, 0)
    crossed = jnp.where(at_end, 0, experts - 1) if kept else experts - 1
    pl.semaphore_wait(barrier, 1 + linked + crossed)
    pair_copy(first, spans[0], 0).start()
    for load in opening[1:]:
        load.wait()
    for p in range(1, steps):
        pair_out[first, spans[p]] = grad[first, other, spans[p]].astype(jnp.float32)
        pair_copy(first, spans[p], p).start()

    def open_link(p):
        link_copy(way_out, first, p, local.at[first, spans[p]]).start()

    sender = at_end & (first != z)
    late_core = 1
    hold = min(2, steps - 1)
    for p in range(steps):
        pair_copy(first, spans[p], p).wait_recv()
        local[first, spans[p]] = local[first, spans[p]] + grad[first, core, spans[p]].astype(jnp.float32)
        if p == 0 and hold:
            pl.when(sender & (core != late_core))(lambda: open_link(0))
        if p == hold and hold:
            for q in range(hold):
                pl.when(sender & (core == late_core))(lambda: open_link(q))
        if 0 < p < hold:
            pl.when(sender & (core != late_core))(lambda: open_link(p))
        elif p >= hold:
            pl.when(sender)(lambda: open_link(p))

    whole = pl.ds(0, rows)

    def give(j):
        load_level(j).wait()
        d = level_of(j)
        pair_out[d] = grad[d, other].astype(jnp.float32)
        pair_copy(d, whole, steps + j - 1).start()

    def take(j):
        d = level_of(j)
        pair_copy(d, whole, steps + j - 1).wait_recv()
        local[d] = local[d] + grad[d, core].astype(jnp.float32)

        @pl.when(at_end & (j < levels - 2))
        def _():
            for p in range(steps):
                link_copy(way_out, d, p, local.at[d, spans[p]]).start()

        @pl.when(at_end & (j == levels - 2))
        def _():
            for p in reversed(range(kept, steps)):
                link_copy(way_out, d, p, local.at[d, spans[p]]).start()

    ints = [
        pltpu.make_async_copy(a, b, load_sem.at[i])
        for i, (a, b) in enumerate(((count_hbm, count_ref), (holder_hbm, holder_ref), (slot_hbm, slot_ref), (step_hbm, step_ref)))
    ]
    for load in ints:
        load.start()
    for i, source in enumerate((hm_hbm, hs_hbm)):
        pltpu.make_async_copy(source, held.at[i], load_sem.at[4]).start()

    if levels > 1:
        give(1)

    @pl.loop(1, levels)
    def _(j):
        @pl.when(j + 1 < levels)
        def _():
            give(j + 1)

        take(j)

    if kept:
        pl.when(near)(lambda: greet(ready_sem))
    for i, source in enumerate((w_hbm, m_hbm, v_hbm)):
        pltpu.make_async_copy(source, wmv.at[i], load_sem.at[5]).start()
    for i, source in enumerate((eg_hbm, ew_hbm)):
        pltpu.make_async_copy(source, blocks.at[i], load_sem.at[6]).start()
    for load in ints:
        load.wait()
    pltpu.make_async_copy(held, held, load_sem.at[4]).wait()

    def moment_copy(target, source):
        return pltpu.make_async_remote_copy(
            src_ref=mom_out.at[target], dst_ref=mom_in.at[source],
            send_sem=mom_send, recv_sem=mom_recv,
            device_id=(dp, target), device_id_type=MESH,
        )

    def picks(owner):
        rank = jnp.int32(0)
        chosen = [jnp.int32(0)] * per_holder
        for b in range(maxb):
            mine = (holder_ref[owner, b] == me) & (b < count_ref[owner])
            for q in range(per_holder):
                chosen[q] = jnp.where(mine & (rank == q), slot_ref[owner, b], chosen[q])
            rank = rank + jnp.where(mine, 1, 0)
        return chosen

    if kept:
        @pl.when(near)
        def _():
            pl.semaphore_wait(ready_sem, experts - 1)
            edge_dp = jnp.where(upper, dp + CORES, dp - CORES)
            pl.semaphore_signal(open_sem, inc=1, device_id=(edge_dp, me), device_id_type=MESH)

        @pl.when(at_end)
        def _():
            pl.semaphore_wait(open_sem, 1)

    for q, slot in enumerate(picks(me)):
        for i in range(2):
            mom_in[me, i, pl.ds(q, 1), :] = held[i, pl.ds(slot, 1), :]

    @pl.loop(1, experts)
    def _(off):
        owner = lax.rem(me + off, experts)
        for q, slot in enumerate(picks(owner)):
            for i in range(2):
                mom_out[owner, i, pl.ds(q, 1), :] = held[i, pl.ds(slot, 1), :]
        moment_copy(owner, me).start()

    def forward(way, j, p):
        d = jnp.where(way == 0, levels - 1 - j, j)
        ahead = jnp.where(way == 0, (d > z) & (z > 0), (d < z) & (z < levels - 1))
        slot = d + 1 - way

        @pl.when(ahead)
        def _():
            block = recv.at[slot, spans[p]]
            copy = link_copy(way, d, p, block)
            copy.wait_recv()
            recv[slot, spans[p]] = recv[slot, spans[p]] + local[d, spans[p]]
            copy.start()

        if p < kept:
            @pl.when((d == z) & (z == jnp.where(way == 0, levels - 2, 1)))
            def _():
                copy = link_copy(way, d, p, recv.at[slot, spans[p]], back_send)
                copy.wait_recv()
                recv[slot, spans[p]] = recv[slot, spans[p]] + local[d, spans[p]]
                copy.start()

    lag = min(LAG, steps)

    @pl.loop(0, levels)
    def _(j):
        for p in range(steps):
            forward(way_out, j, p)
            if p >= lag:
                forward(1 - way_out, j, p - lag)
            else:
                @pl.when(j > 0)
                def _():
                    forward(1 - way_out, j - 1, p - lag + steps)

    if experts > 1:
        others = mom_in.at[pl.ds(0, experts - 1)]
        pltpu.make_async_copy(others, others, mom_recv).wait()
        others = mom_out.at[pl.ds(0, experts - 1)]
        pltpu.make_async_copy(others, others, mom_send).wait()

    owned = count_ref[me]
    for b in range(maxb):
        holder = holder_ref[me, b]
        rank = jnp.int32(0)
        for earlier in range(b):
            rank = rank + jnp.where((holder_ref[me, earlier] == holder) & (earlier < owned), 1, 0)
        rank = jnp.minimum(rank, per_holder - 1)
        for i in range(2):
            blocks[2 + i, pl.ds(b, 1), :] = mom_in[holder, i, pl.ds(rank, 1), :]
    taken = blocks.at[pl.ds(0, 2)]
    pltpu.make_async_copy(taken, taken, load_sem.at[6]).wait()
    width = blocks.shape[2]
    live = lax.broadcasted_iota(jnp.int32, (maxb, 128), 0) < owned
    acc = jnp.zeros((maxb, 128), jnp.float32)
    for i in range(width // 128):
        span = pl.ds(i * 128, 128)
        g = jnp.where(live, blocks[0, :, span], 0.0)
        w = blocks[1, :, span]
        blocks[0, :, span] = g
        blocks[1, :, span] = jnp.where(live, (1.0 - learn_rate * decay_rate) * w, w)
        blocks[2, :, span] = jnp.where(live, beta_first * blocks[2, :, span], 0.0)
        blocks[3, :, span] = jnp.where(live, beta_second * blocks[3, :, span], 0.0)
        acc = acc + g * g
    row = jnp.sum(acc, axis=0, keepdims=True)
    pltpu.make_async_copy(wmv, wmv, load_sem.at[5]).wait()
    for i, scale in enumerate((1.0 - learn_rate * decay_rate, beta_first, beta_second)):
        wmv[i] = wmv[i] * scale
    step = step_ref[0]
    one = jnp.ones((1, 128), jnp.float32)
    first_left = one * (1.0 - power(beta_first, step))
    second_root = jnp.sqrt(one * (1.0 - power(beta_second, step)))
    scale_ref[2:3] = learn_rate * second_root / first_left
    scale_ref[3:4] = adam_epsilon * second_root

    early = 1 - way_out
    inner = jnp.where(upper, z > 0, z < levels - 1)
    outer = jnp.where(upper, z < levels - 1, z > 0)
    part[...] = row

    def square(ref, at):
        g = ref[at]
        col = jnp.sum(g * g, axis=0, keepdims=True)
        for i in range(g.shape[1] // 128):
            part[...] = part[...] + col[:, i * 128:(i + 1) * 128]

    for p in range(steps):
        taken = near if p < kept else False

        @pl.when(inner & jnp.logical_not(taken))
        def _():
            link_copy(early, z, p, recv.at[z + 1 - early, spans[p]]).wait_recv()
            sum_ref[spans[p]] = local[z, spans[p]] + recv[z + 1 - early, spans[p]]

        @pl.when(jnp.logical_not(inner))
        def _():
            sum_ref[spans[p]] = local[z, spans[p]]

    if kept:
        @pl.when(at_end)
        def _():
            d = level_of(levels - 2)
            slot = d + 1 - early
            for p in range(kept):
                block = recv.at[slot, spans[p]]
                link_copy(early, d, p, block).wait_recv()
                recv[slot, spans[p]] = recv[slot, spans[p]] + local[d, spans[p]]
                square(recv, (slot, spans[p]))

    def last(p):
        link_copy(way_out, z, p, recv.at[z + 1 - way_out, spans[p]]).wait_recv()

    for p in reversed(range(steps)):
        taken = near if p < kept else False

        @pl.when(outer & jnp.logical_not(taken))
        def _():
            last(p)
            sum_ref[spans[p]] = sum_ref[spans[p]] + recv[z + 1 - way_out, spans[p]]

        @pl.when(jnp.logical_not(taken))
        def _():
            square(sum_ref, spans[p])

    inside = devices - 2 * CORES * experts if kept else devices
    index = dp * experts + me - (CORES * experts if kept else 0)

    def part_copy(target_dp, target_me):
        return pltpu.make_async_remote_copy(
            src_ref=part, dst_ref=parts.at[index],
            send_sem=part_send, recv_sem=part_recv,
            device_id=(target_dp, target_me), device_id_type=MESH,
        )

    def spread():
        parts[index] = part[...]
        if devices <= 64:
            for far in far_first(levels):
                side = lax.rem(z + far, levels) * CORES
                for off in far_first(experts):
                    target = lax.rem(me + off, experts)
                    for swap in range(CORES):
                        if far or off or swap:
                            part_copy(side + lax.rem(core + swap, CORES), target).start()
        else:
            @pl.loop(1, devices)
            def _(off):
                target = lax.rem(dp * experts + me + off, devices)
                part_copy(target // experts, lax.rem(target, experts)).start()

    if kept:
        edge = pltpu.make_async_remote_copy(
            src_ref=part, dst_ref=edge_part, send_sem=edge_sem.at[0], recv_sem=edge_sem.at[1],
            device_id=(jnp.where(upper, dp - CORES, dp + CORES), me), device_id_type=MESH,
        )

        @pl.when(at_end)
        def _():
            edge.start()
            d = level_of(levels - 2)
            for p in reversed(range(kept)):
                link_copy(way_out, d, p, recv.at[d + 1 - early, spans[p]]).start()

        @pl.when(near)
        def _():
            edge.wait_recv()
            part[...] = part[...] + edge_part[...]

        pl.when(jnp.logical_not(at_end))(spread)
    else:
        spread()

    everyone = parts.at[pl.ds(0, devices - 1)]
    if kept:
        @pl.when(at_end)
        def _():
            everything = parts.at[pl.ds(0, inside)]
            pltpu.make_async_copy(everything, everything, part_recv).wait()

        @pl.when(jnp.logical_not(at_end))
        def _():
            others = parts.at[pl.ds(0, inside - 1)]
            pltpu.make_async_copy(others, others, part_recv).wait()
    else:
        pltpu.make_async_copy(everyone, everyone, part_recv).wait()
    total = jnp.sum(jnp.sum(parts[pl.ds(0, inside)], axis=0), axis=1, keepdims=True)
    factor = jnp.broadcast_to(jnp.minimum(1.0, clip_norm / (jnp.sqrt(total) + 1e-06)), (1, 128))
    scale_ref[0:1] = (1.0 - beta_first) * factor
    scale_ref[1:2] = (1.0 - beta_second) ** 0.5 * factor

    def finish(span, g):
        m = wmv[1, span] + scale_ref[0:1, 0:1] * g
        s = scale_ref[1:2, 0:1] * g
        v = wmv[2, span] + s * s
        wmv[1, span] = m
        wmv[2, span] = v
        wmv[0, span] = wmv[0, span] - scale_ref[2:3, 0:1] * m / (v * lax.rsqrt(v) + scale_ref[3:4, 0:1])

    for p in range(kept, steps):
        finish(spans[p], sum_ref[spans[p]])
    for i in range(width // 128):
        span = pl.ds(i * 128, 128)
        g = blocks[0, :, span]
        m = blocks[2, :, span] + scale_ref[0:1, 0:1] * g
        s = scale_ref[1:2, 0:1] * g
        v = blocks[3, :, span] + s * s
        blocks[2, :, span] = m
        blocks[3, :, span] = v
        blocks[1, :, span] = blocks[1, :, span] - scale_ref[2:3, 0:1] * m / (jnp.sqrt(v) + scale_ref[3:4, 0:1])
    if kept:
        @pl.when(jnp.logical_not(near))
        def _():
            for p in range(kept):
                finish(spans[p], sum_ref[spans[p]])

    pltpu.make_async_copy(pair_out, pair_out, pair_send).wait()
    if levels > 1:
        sent = local.at[pl.ds(0, levels - 1)]
        pltpu.make_async_copy(sent, sent, link_send).wait()
    if kept:
        @pl.when(at_end)
        def _():
            edge.wait_send()

        @pl.when(jnp.logical_not(at_end))
        def _():
            pltpu.make_async_copy(everyone, everyone, part_send).wait()

        @pl.when(near)
        def _():
            back = local.at[0, pl.ds(0, sum(size for _, size in cuts[:kept]))]
            pltpu.make_async_copy(back, back, back_send).wait()
            for p in reversed(range(kept)):
                last(p)
                finish(spans[p], recv[z + 1 - way_out, spans[p]])
    else:
        pltpu.make_async_copy(everyone, everyone, part_send).wait()


def write(parts, wmv, blocks, ow_hbm, om_hbm, ov_hbm, oew_hbm, oem_hbm, oes_hbm, sem, block_sem):
    size = wmv.shape[1] // parts
    for k in range(parts):
        span = pl.ds(k * size, size)
        for i, dst in enumerate((ow_hbm, om_hbm, ov_hbm)):
            pltpu.make_async_copy(wmv.at[i, span], dst.at[span], sem).start()
    for i, dst in enumerate((oew_hbm, oem_hbm, oes_hbm)):
        pltpu.make_async_copy(blocks.at[i + 1], dst, block_sem).start()
    done = blocks.at[pl.ds(1, 3)]
    pltpu.make_async_copy(wmv, wmv, sem).wait()
    pltpu.make_async_copy(done, done, block_sem).wait()


def cut_rows(rows):
    unit = rows // 6 // 16 * 16
    if not unit or rows % 16:
        return ((0, rows),)
    half = unit // 2 // 16 * 16
    sizes = ([half, unit - half] if half else [unit]) + [unit] * ((rows - unit) // unit)
    if rows > sum(sizes):
        sizes.append(rows - sum(sizes))
    return tuple((sum(sizes[:i]), sizes[i]) for i in range(len(sizes)))


def make_body(mesh):
    n_dp = mesh.shape["dp"]
    experts = mesh.shape["expert"]
    levels = n_dp // CORES

    def body(ag, aw, am, av, eg, ew, hm, hs, count, holder, slot, step):
        depth, cols = ag.shape[1], ag.shape[2]
        rows = depth // n_dp
        cuts = cut_rows(rows)
        maxb, width = eg.shape[2], eg.shape[3]
        slots = hm.shape[1]
        per_holder = max(1, maxb // experts)
        f32 = jnp.float32
        hbm = pl.BlockSpec(memory_space=pltpu.HBM)
        vmem = pl.BlockSpec(memory_space=pltpu.VMEM)
        shape = jax.ShapeDtypeStruct
        moved = (experts, 2, per_holder, width)
        wmv, blocks = pl.pallas_call(
            functools.partial(kernel, levels, experts, per_holder, cuts),
            out_shape=[pltpu.VMEM(s, f32) for s in ((3, rows, cols), (4, maxb, width))],
            in_specs=[hbm] * 12,
            out_specs=[vmem] * 2,
            scratch_shapes=[
                pltpu.VMEM((rows, cols), f32), pltpu.VMEM((4, 128), f32),
                pltpu.VMEM((levels, CORES, rows, cols), ag.dtype),
                pltpu.VMEM((levels, rows, cols), f32),
                pltpu.VMEM((levels, rows, cols), f32),
                pltpu.VMEM((levels + 1, rows, cols), f32),
                pltpu.VMEM((2, slots, width), f32),
                pltpu.VMEM(moved, f32), pltpu.VMEM(moved, f32),
                pltpu.VMEM((1, 128), f32), pltpu.VMEM((n_dp * experts, 1, 128), f32), pltpu.VMEM((1, 128), f32),
                pltpu.SMEM(count.shape, jnp.int32), pltpu.SMEM(holder.shape, jnp.int32),
                pltpu.SMEM(slot.shape, jnp.int32), pltpu.SMEM(step.shape, jnp.int32),
            ],
            compiler_params=pltpu.CompilerParams(
                collective_id=0, has_side_effects=True, vmem_limit_bytes=LIMIT
            ),
        )(
            *(pltpu.with_memory_space_constraint(x, pltpu.HBM) for x in (
                ag.reshape(levels, CORES, rows, cols), eg[0, 0], ew[0, 0],
                aw, am, av, hm[0], hs[0], count, holder, slot,
            )),
            step,
        )
        outs = pl.pallas_call(
            functools.partial(write, WRITES if rows % (8 * WRITES) == 0 else 1),
            out_shape=[shape((rows, cols), f32)] * 3 + [shape((maxb, width), f32)] * 3,
            in_specs=[vmem] * 2,
            out_specs=[hbm] * 6,
            scratch_shapes=[pltpu.SemaphoreType.DMA(()), pltpu.SemaphoreType.DMA(())],
            compiler_params=pltpu.CompilerParams(vmem_limit_bytes=16 * 1024 * 1024),
        )(wmv, blocks)
        return tuple(outs[:3]) + tuple(o[None, None] for o in outs[3:])

    return body


def solution(mesh):
    matrix = P("dp", "expert")
    blocks = P("dp", "expert", None, None)
    held = P("dp", "expert", None)
    return jax.shard_map(
        make_body(mesh),
        mesh=mesh,
        in_specs=(P("dp", None, "expert"), matrix, matrix, matrix, blocks, blocks, held, held, P(), P(), P(), P()),
        out_specs=(matrix, matrix, matrix, blocks, blocks, blocks),
        check_vma=False,
    )
```
